32 devices in a mesh: rep: 2 (over x), dp: 16 (over y, z, core).
Axes of the slice: x: 2, y: 2, z: 4, core: 2. Of those that a mesh axis runs over, the one named last changes fastest.
Arguments:
- g_w_gate: bfloat16 [32, 2, 1152, 4608], P(('rep', 'dp')), parts along dimension 0
- g_w_up: bfloat16 [32, 2, 1152, 4608], P(('rep', 'dp')), parts along dimension 0
- g_w_down: bfloat16 [32, 2, 4608, 1152], P(('rep', 'dp')), parts along dimension 0
- w_gate: bfloat16 [2, 1152, 4608], replicated
- w_up: bfloat16 [2, 1152, 4608], replicated
- w_down: bfloat16 [2, 4608, 1152], replicated
- m_w_gate: float32 [2, 1152, 4608], P(None, 'dp')
- m_w_up: float32 [2, 1152, 4608], P(None, 'dp')
- m_w_down: float32 [2, 4608, 1152], P(None, 'dp')
- v_w_gate: float32 [2, 1152, 4608], P(None, 'dp')
- v_w_up: float32 [2, 1152, 4608], P(None, 'dp')
- v_w_down: float32 [2, 4608, 1152], P(None, 'dp')
Outputs:
- output 1: bfloat16 [4, 1152, 4608], P('rep'), parts along dimension 0
- output 2: bfloat16 [4, 1152, 4608], P('rep'), parts along dimension 0
- output 3: bfloat16 [4, 4608, 1152], P('rep'), parts along dimension 0
- output 4: float32 [4, 1152, 4608], P('rep', 'dp'), parts along dimension 0
- output 5: float32 [4, 1152, 4608], P('rep', 'dp'), parts along dimension 0
- output 6: float32 [4, 4608, 1152], P('rep', 'dp'), parts along dimension 0
- output 7: float32 [4, 1152, 4608], P('rep', 'dp'), parts along dimension 0
- output 8: float32 [4, 1152, 4608], P('rep', 'dp'), parts along dimension 0
- output 9: float32 [4, 4608, 1152], P('rep', 'dp'), parts along dimension 0
There are 2 independent parts. The reference program is written for one: setup_inputs(seed, part) draws one part's arguments, and reference() takes and returns one part's arrays. A program takes and returns all parts, laid end to end along the dimension named above; an argument that names none is the same for every part.
All inputs are finite; a program needn't handle non-finite values.
Results may differ from the reference program's by a relative error of at most 0.022.
Values are sent between devices in bfloat16 or wider.
A program may use at most 2 GiB of HBM per device.

```python
import jax
import jax.numpy as jnp
from jax import lax

DEVICES = 16
D = 1152
FF = 4608
LAYERS = 2
NAMES = ("w_gate", "w_up", "w_down")
SHAPES = {"w_gate": (LAYERS, D, FF), "w_up": (LAYERS, D, FF), "w_down": (LAYERS, FF, D)}


def setup_inputs(seed: int = 0, part: int = 0) -> dict:
    kz, *keys = jax.random.split(jax.random.key(seed), 1 + 5 * len(NAMES))
    loud = 2.0 ** jax.random.uniform(kz, (), jnp.float32, -1.0, 1.0)
    drawn = {}
    for name, key, both in zip(NAMES, keys[:3], keys[3:6], strict=True):
        own = jax.random.normal(jax.random.fold_in(key, part), (DEVICES, *SHAPES[name]), jnp.float32)
        shared = jax.random.normal(jax.random.fold_in(both, part), SHAPES[name], jnp.float32)
        drawn["g_" + name] = (loud * (0.7 * shared / DEVICES + 0.7 * own * DEVICES**-0.5)).astype(jnp.bfloat16)
    for name, key in zip(NAMES, keys[6:9], strict=True):
        drawn[name] = (jax.random.normal(key, SHAPES[name], jnp.float32) * SHAPES[name][1] ** -0.5).astype(jnp.bfloat16)
    for name, key in zip(NAMES, keys[9:12], strict=True):
        drawn["m_" + name] = loud * 0.5 * jax.random.normal(key, SHAPES[name], jnp.float32)
    for name, key in zip(NAMES, keys[12:15], strict=True):
        drawn["v_" + name] = loud * loud * jax.random.uniform(key, SHAPES[name], jnp.float32, 0.5, 1.5)
    return drawn


def adamw(w, m, v, g):
    m = 0.9 * m + 0.1 * g
    v = 0.95 * v + 0.05 * g * g
    step = m * lax.rsqrt(v + 1e-8) + 0.1 * w
    return (w - 0.02 * step).astype(jnp.bfloat16), m, v


def reference(g_w_gate, g_w_up, g_w_down, w_gate, w_up, w_down, m_w_gate, m_w_up, m_w_down, v_w_gate, v_w_up, v_w_down):
    def total(terms):
        return lax.scan(lambda so_far, term: (so_far + term.astype(jnp.float32), None), jnp.zeros(terms.shape[1:], jnp.float32), terms)[0]

    gradients = [total(terms).astype(jnp.bfloat16).astype(jnp.float32) for terms in (g_w_gate, g_w_up, g_w_down)]
    new = [
        adamw(w.astype(jnp.float32), m, v, g)
        for w, m, v, g in zip((w_gate, w_up, w_down), (m_w_gate, m_w_up, m_w_down), (v_w_gate, v_w_up, v_w_down), gradients, strict=True)
    ]
    return tuple(one[which] for which in range(3) for one in new)
```

```python
import jax
import jax.numpy as jnp
from jax import lax
from jax.experimental import pallas as pl
from jax.experimental.pallas import tpu as pltpu
from jax.sharding import PartitionSpec as P

F32, BF16 = jnp.float32, jnp.bfloat16
CHIPS = 8
MESH = pl.DeviceIdType.MESH


def chip_at(p):
    return p + lax.div(p, 4) * (11 - 2 * p)


def kernel(*refs):
    terms, weights, ms, vs = (refs[i : i + 3] for i in (0, 3, 6, 9))
    new_w, new_m, new_v, partner = (refs[i : i + 3] for i in (12, 15, 18, 21))
    wide, tall, own_wide, own_tall, w_wide, w_tall, m_wide, m_tall, v_wide, v_tall = refs[24:34]
    load_sem, state_sem, out_sem, d2d_send, d2d_recv, rs_send, rs_recv, ag_send, ag_recv, pair_send, pair_recv = refs[34:]

    me = lax.axis_index("dp")
    chip, core = lax.div(me, 2), lax.rem(me, 2)
    p = chip_at(chip)
    other = {"dp": 2 * chip + 1 - core}
    up = {"dp": 2 * chip_at(lax.rem(p + 1, CHIPS)) + core}
    down = {"dp": 2 * chip_at(lax.rem(p + CHIPS - 1, CHIPS)) + core}
    ahead = (up, down)

    barrier = pltpu.get_barrier_semaphore()
    for device in (up, down, other):
        pl.semaphore_signal(barrier, inc=1, device_id=device, device_id_type=MESH)
    pl.semaphore_wait(barrier, 3)

    def part(ref, index, way, which):
        if which == 2:
            return ref.at[(*index, way)]
        return ref.at[(*index, slice(None), pl.ds(2304 * way, 2304))]

    tasks = [(2 * which + layer, which, layer, way) for which in range(3) for layer in range(2) for way in range(2)]

    def block_of(way, back):
        return chip_at(lax.rem(p + CHIPS - back, CHIPS) if way == 0 else lax.rem(p + back, CHIPS))

    def sums(unit, which, way, k):
        return tall.at[unit - 4, way, k] if which == 2 else wide.at[unit, way, k]

    def to_partner(k, unit, which, layer, way):
        block = block_of(way, lax.rem(k + 1, CHIPS))
        return pltpu.make_async_remote_copy(
            part(terms[which], (layer, block, 1 - core), way, which),
            part(partner[which], (layer, block), way, which),
            d2d_send.at[unit, k, way],
            d2d_recv.at[unit, k, way],
            device_id=other,
            device_id_type=MESH,
        )

    def load(k, unit, which, layer, way):
        block = block_of(way, lax.rem(k + 1, CHIPS))
        mine = own_tall if which == 2 else own_wide
        return (
            pltpu.make_async_copy(part(terms[which], (layer, block, core), way, which), mine.at[way, 0], load_sem.at[way, 0]),
            pltpu.make_async_copy(part(partner[which], (layer, block), way, which), mine.at[way, 1], load_sem.at[way, 1]),
        )

    def start_load(k, task):
        to_partner(k, *task).wait_recv()
        for copy in load(k, *task):
            copy.start()

    def hop(k, unit, which, layer, way):
        return pltpu.make_async_remote_copy(
            sums(unit, which, way, k),
            sums(unit, which, way, k + 1),
            rs_send.at[unit, k, way],
            rs_recv.at[unit, k, way],
            device_id=ahead[way],
            device_id_type=MESH,
        )

    def state(unit, which, layer, way):
        w, m, v = (w_tall, m_tall, v_tall) if which == 2 else (w_wide, m_wide, v_wide)
        i = unit - 4 if which == 2 else unit
        return w.at[i, way], m.at[i, way], v.at[i, way]

    def load_state(unit, which, layer, way):
        w, m, v = state(unit, which, layer, way)
        return (
            pltpu.make_async_copy(part(weights[which], (layer, chip, core), way, which), w, state_sem.at[unit, way, 0]),
            pltpu.make_async_copy(part(ms[which], (layer,), way, which), m, state_sem.at[unit, way, 1]),
            pltpu.make_async_copy(part(vs[which], (layer,), way, which), v, state_sem.at[unit, way, 2]),
        )

    def store_state(unit, which, layer, way):
        _, m, v = state(unit, which, layer, way)
        return (
            pltpu.make_async_copy(sums(unit, which, way, 7), part(new_w[which], (layer, chip, core), way, which), out_sem.at[unit, way, 0]),
            pltpu.make_async_copy(m, part(new_m[which], (layer,), way, which), out_sem.at[unit, way, 1]),
            pltpu.make_async_copy(v, part(new_v[which], (layer,), way, which), out_sem.at[unit, way, 2]),
        )

    def forward(k, unit, which, layer, way, first):
        where = part(new_w[which], (layer, block_of(way, k), core), way, which)
        return pltpu.make_async_remote_copy(
            sums(unit, which, way, 7) if first else where,
            where,
            ag_send.at[unit, k, way],
            ag_recv.at[unit, k, way],
            device_id=ahead[way],
            device_id_type=MESH,
        )

    def arrival(k, unit, which, layer, way):
        where = part(new_w[which], (layer, block_of(way, k + 1), core), way, which)
        return pltpu.make_async_remote_copy(
            where, where, ag_send.at[unit, k, way], ag_recv.at[unit, k, way], device_id=ahead[way], device_id_type=MESH
        )

    def hand_over(k, unit, which, layer, way, first):
        where = part(new_w[which], (layer, block_of(way, k), core), way, which)
        return pltpu.make_async_remote_copy(
            sums(unit, which, way, 7) if first else where,
            where,
            pair_send.at[unit, k, way],
            pair_recv.at[unit, k, way],
            device_id=other,
            device_id_type=MESH,
        )

    def taken_over(k, unit, which, layer, way):
        where = part(new_w[which], (layer, block_of(way, k), 1 - core), way, which)
        return pltpu.make_async_remote_copy(
            where, where, pair_send.at[unit, k, way], pair_recv.at[unit, k, way], device_id=other, device_id_type=MESH
        )

    def columns(which):
        return 128 if which == 2 else 256

    def reduce_step(k, first):
        for i, task in enumerate(tasks):
            unit, which, layer, way = task
            if i + 1 < len(tasks):
                start_load(k, tasks[i + 1])
            for copy in load(k, *task):
                copy.wait()
            if not first:
                hop(k - 1, *task).wait_recv()
            total = sums(unit, which, way, k)
            mine = (own_tall if which == 2 else own_wide).at[way]
            size = columns(which)

            def add(j, _, total=total, mine=mine, size=size):
                at = (slice(None), pl.ds(pl.multiple_of(j * size, size), size))
                x = mine[(0, *at)].astype(F32) + mine[(1, *at)].astype(F32)
                if not first:
                    x = x + total[at].astype(F32)
                total[at] = x.astype(BF16)
                return 0

            lax.fori_loop(0, 9, add, 0)
            hop(k, *task).start()
            if i + 1 == len(tasks):
                start_load(k + 1, tasks[0])

    for k in range(2):
        for task in tasks:
            to_partner(k, *task).start()
    start_load(0, tasks[0])
    reduce_step(0, True)

    def reduce_loop(k, _):
        for task in tasks:
            to_partner(k + 1, *task).start()
        reduce_step(k, False)
        return 0

    for task in tasks:
        for copy in load_state(*task):
            copy.start()
    lax.fori_loop(1, 7, reduce_loop, 0)

    for i, task in enumerate(tasks):
        unit, which, layer, way = task
        if i + 1 < len(tasks):
            start_load(7, tasks[i + 1])
        for copy in load(7, *task) + load_state(*task):
            copy.wait()
        hop(6, *task).wait_recv()
        total = sums(unit, which, way, 7)
        mine = (own_tall if which == 2 else own_wide).at[way]
        w_ref, m_ref, v_ref = state(*task)
        size = columns(which)

        def adamw(j, _, total=total, mine=mine, w_ref=w_ref, m_ref=m_ref, v_ref=v_ref, size=size):
            at = (slice(None), pl.ds(pl.multiple_of(j * size, size), size))
            g = mine[(0, *at)].astype(F32) + mine[(1, *at)].astype(F32) + total[at].astype(F32)
            g = g.astype(BF16).astype(F32)
            w = w_ref[at].astype(F32)
            m = 0.9 * m_ref[at] + 0.1 * g
            v = 0.95 * v_ref[at] + 0.05 * g * g
            step = m * lax.rsqrt(v + 1e-8) + 0.1 * w
            total[at] = (w - 0.02 * step).astype(BF16)
            m_ref[at] = m
            v_ref[at] = v
            return 0

        lax.fori_loop(0, 9, adamw, 0)
        forward(0, *task, True).start()
        hand_over(0, *task, True).start()
        for copy in store_state(*task):
            copy.start()

    def gather_loop(k, _):
        for task in tasks:
            arrival(k - 1, *task).wait_recv()
            forward(k, *task, False).start()
            hand_over(k, *task, False).start()
        return 0

    lax.fori_loop(1, 7, gather_loop, 0)
    for task in tasks:
        arrival(6, *task).wait_recv()
        hand_over(7, *task, False).start()

    for task in tasks:
        for copy in store_state(*task):
            copy.wait()

    def drain(k, _):
        for task in tasks:
            hop(k, *task).wait_send()
            forward(k, *task, False).wait_send()
        return 0

    def drain_pair(k, _):
        for task in tasks:
            to_partner(k, *task).wait_send()
            hand_over(k, *task, False).wait_send()
            taken_over(k, *task).wait_recv()
        return 0

    lax.fori_loop(0, 7, drain, 0)
    lax.fori_loop(0, 8, drain_pair, 0)


def solution(mesh):
    def step(*arrays):
        terms = [arrays[0].reshape(2, 8, 2, 72, 4608), arrays[1].reshape(2, 8, 2, 72, 4608), arrays[2].reshape(2, 8, 2, 2, 144, 1152)]
        weights = [arrays[3].reshape(2, 8, 2, 72, 4608), arrays[4].reshape(2, 8, 2, 72, 4608), arrays[5].reshape(2, 8, 2, 2, 144, 1152)]
        moments = [a if i % 3 < 2 else a.reshape(2, 2, 144, 1152) for i, a in enumerate(arrays[6:])]
        wide_w = jax.ShapeDtypeStruct((2, 8, 2, 72, 4608), BF16)
        tall_w = jax.ShapeDtypeStruct((2, 8, 2, 2, 144, 1152), BF16)
        wide_m = jax.ShapeDtypeStruct((2, 72, 4608), F32)
        tall_m = jax.ShapeDtypeStruct((2, 2, 144, 1152), F32)
        wide_p = jax.ShapeDtypeStruct((2, 8, 72, 4608), BF16)
        tall_p = jax.ShapeDtypeStruct((2, 8, 2, 144, 1152), BF16)
        wide, tall = (72, 2304), (144, 1152)
        dma = pltpu.SemaphoreType.DMA
        out = pl.pallas_call(
            kernel,
            out_shape=(wide_w, wide_w, tall_w, *(wide_m, wide_m, tall_m) * 2, wide_p, wide_p, tall_p),
            in_specs=[pl.BlockSpec(memory_space=pl.ANY)] * 12,
            out_specs=[pl.BlockSpec(memory_space=pl.ANY)] * 12,
            scratch_shapes=[
                pltpu.VMEM((4, 2, 8, *wide), BF16),
                pltpu.VMEM((2, 2, 8, *tall), BF16),
                pltpu.VMEM((2, 2, *wide), BF16),
                pltpu.VMEM((2, 2, *tall), BF16),
                pltpu.VMEM((4, 2, *wide), BF16),
                pltpu.VMEM((2, 2, *tall), BF16),
                pltpu.VMEM((4, 2, *wide), F32),
                pltpu.VMEM((2, 2, *tall), F32),
                pltpu.VMEM((4, 2, *wide), F32),
                pltpu.VMEM((2, 2, *tall), F32),
                dma((2, 2)),
                dma((6, 2, 3)),
                dma((6, 2, 3)),
                dma((6, 8, 2)),
                dma((6, 8, 2)),
                dma((6, 7, 2)),
                dma((6, 7, 2)),
                dma((6, 7, 2)),
                dma((6, 7, 2)),
                dma((6, 8, 2)),
                dma((6, 8, 2)),
            ],
            compiler_params=pltpu.CompilerParams(collective_id=0, has_side_effects=True, vmem_limit_bytes=62 * 1024 * 1024),
        )(*terms, *weights, *moments)
        shapes = [a.shape for a in arrays[3:]]
        return tuple(a.reshape(s) for a, s in zip(out[:9], shapes, strict=True))

    all_of, cut = P(None, None, None), P(None, "dp", None)
    return jax.shard_map(
        step,
        mesh=mesh,
        in_specs=(P(("rep", "dp"), None, None, None),) * 3 + (all_of,) * 3 + (cut,) * 6,
        out_specs=(P("rep", None, None),) * 3 + (P("rep", "dp", None),) * 6,
        check_vma=False,
    )
```

```python
import jax
import jax.numpy as jnp
from jax import lax
from jax.experimental import pallas as pl
from jax.experimental.pallas import tpu as pltpu
from jax.sharding import PartitionSpec as P

F32, BF16 = jnp.float32, jnp.bfloat16
MESH = pl.DeviceIdType.MESH
UNITS = 24
ROWS, A, B, LANES = 72, 40, 32, 1152
LAG, B_STEP, B_OWN, B_OTHER, HAND, B_FIRST = 2, 4, 4, 5, 10, False


def lanes(body):
    def at(j, _):
        body(pl.ds(pl.multiple_of(j * 384, 384), 384))
        return 0

    lax.fori_loop(0, 3, at, 0)


def kernel(*refs):
    terms, weights, ms, vs = (refs[i : i + 3] for i in (0, 3, 6, 9))
    new_w, new_m, new_v = (refs[i : i + 3] for i in (12, 15, 18))
    partner, over_y = refs[21:23]
    xa, xb, out_y, out_z, in_z, la, lb, t_in, a_in, b_in, wa, wb, mv = refs[23:36]
    (
        pair_send, pair_recv, t_load, a_load, b_load, mv_load, wa_load, wb_load, sta, stb, own_a, own_b,
        y_send, y_recv, z_send, z_recv, xa_send, xa_recv, xb_send, xb_recv,
        ga_send, ga_recv, gb_send, gb_recv, ya_send, ya_recv, yb_send, yb_recv, hand_send, hand_recv,
    ) = refs[36:]

    me = lax.axis_index("dp")
    core = lax.rem(me, 2)
    z = lax.rem(lax.div(me, 2), 4)
    y = lax.div(me, 8)
    other = {"dp": me + 1 - 2 * core}
    across = {"dp": me + 8 - 16 * y}
    ahead = ({"dp": me + 2}, {"dp": me - 2})
    place = (z, 3 - z)

    barrier = pltpu.get_barrier_semaphore()
    for device in (other, across):
        pl.semaphore_signal(barrier, inc=1, device_id=device, device_id_type=MESH)
    for way in range(2):

        @pl.when(place[way] < 3)
        def _(way=way):
            pl.semaphore_signal(barrier, inc=1, device_id=ahead[way], device_id_type=MESH)

    pl.semaphore_wait(barrier, 2 + lax.div(z + 2, 3) + lax.div(5 - z, 3))

    def z_of(way, b):
        return b if way == 0 else 3 - b

    def each(u, body):
        for which in range(3):

            @pl.when(lax.div(u, 8) == which)
            def _(which=which):
                body(which, lax.rem(lax.div(u, 4), 2), lax.rem(u, 4))

    def cut(ref, which, lead, q, first, count):
        if which == 2:
            return ref.at[(*lead, q, pl.ds(first, count))]
        return ref.at[(*lead, pl.ds(first, count), pl.ds(pl.multiple_of(q * LANES, 128), LANES))]

    def send(source, target, sent, received, device):
        pltpu.make_async_remote_copy(source, target, sent, received, device_id=device, device_id_type=MESH).start()

    def arrived(like, sem, device=other):
        pltpu.make_async_remote_copy(like, like, sem, sem, device_id=device, device_id_type=MESH).wait_recv()

    def copied(like, sem):
        pltpu.make_async_copy(like, like, sem).wait()

    def to_partner(u):
        def go(which, layer, q):
            source = cut(terms[which], which, (layer, slice(None), slice(None), 1 - core), q, 0, ROWS)
            send(source, partner.at[u], pair_send.at[u], pair_recv.at[u], other)

        each(u, go)

    def load_t(u):
        arrived(partner.at[u], pair_recv.at[u])

        def go(which, layer, q):
            source = cut(terms[which], which, (layer, 1 - y, slice(None), core), q, 0, A)
            pltpu.make_async_copy(source, t_in.at[0], t_load.at[0]).start()

        each(u, go)
        pltpu.make_async_copy(partner.at[u, 1 - y, :, pl.ds(0, A)], t_in.at[1], t_load.at[1]).start()

    def sum_t(u, b):
        if b == 0:
            for i in range(2):
                copied(t_in.at[i], t_load.at[i])

        def body(c):
            out_y[u, b, :, c] = (t_in[0, b, :, c].astype(F32) + t_in[1, b, :, c].astype(F32)).astype(BF16)

        lanes(body)
        send(out_y.at[u, b], over_y.at[u, b], y_send.at[u], y_recv.at[u], across)

    def load_a(u):
        arrived(over_y.at[u], y_recv.at[u], across)

        def go(which, layer, q):
            source = cut(terms[which], which, (layer, y, slice(None), core), q, 0, A)
            pltpu.make_async_copy(source, a_in.at[0], a_load.at[0]).start()

        each(u, go)
        pltpu.make_async_copy(partner.at[u, y, :, pl.ds(0, A)], a_in.at[1], a_load.at[1]).start()
        pltpu.make_async_copy(over_y.at[u], a_in.at[2], a_load.at[2]).start()

    def sum_a(u, first, count):
        if first == 0:
            for i in range(3):
                copied(a_in.at[i], a_load.at[i])

        def one(b, _):
            def body(c):
                la[lax.rem(u, 3), b, :, c] = (
                    a_in[0, b, :, c].astype(F32) + a_in[1, b, :, c].astype(F32) + a_in[2, b, :, c].astype(F32)
                )

            lanes(body)
            return 0

        lax.fori_loop(first, first + count, one, 0)

    def load_b(u):
        def go(which, layer, q):
            source = cut(terms[which], which, (layer, slice(None), slice(None), core), q, A, B)
            pltpu.make_async_copy(source, b_in.at[0], b_load.at[0]).start()

        each(u, go)
        pltpu.make_async_copy(partner.at[u, :, :, pl.ds(A, B)], b_in.at[1], b_load.at[1]).start()

    def sum_b(u, first, count):
        if first == 0:
            for i in range(2):
                copied(b_in.at[i], b_load.at[i])

        def one(n, _):
            b, s = lax.div(n, 2), lax.rem(n, 2)

            def body(c):
                lb[lax.rem(u, 3), b, s, :, c] = b_in[0, s, b, :, c].astype(F32) + b_in[1, s, b, :, c].astype(F32)

            lanes(body)
            return 0

        lax.fori_loop(2 * first, 2 * (first + count), one, 0)

    def hop_a(u, way, b):
        i = place[way]
        x = xa.at[u, way, b - 1]
        mine = la.at[lax.rem(u, 3), z_of(way, b)]

        @pl.when(i == 0)
        def _():
            def body(c):
                x[:, c] = mine[:, c].astype(BF16)

            lanes(body)

        @pl.when(i > 0)
        def _():
            arrived(x, xa_recv.at[u, way, b - 1])

            def body(c):
                x[:, c] = (mine[:, c] + x[:, c].astype(F32)).astype(BF16)

            lanes(body)

        send(x, x, xa_send.at[u], xa_recv.at[u, way, b - 1], ahead[way])

    def hop_b(u, way, b):
        i = place[way]
        x = xb.at[u, way, b - 1]
        mine = lb.at[lax.rem(u, 3), z_of(way, b)]

        @pl.when(i == 0)
        def _():
            def body(c):
                for s in range(2):
                    x[s, :, c] = mine[s, :, c].astype(BF16)

            lanes(body)

        @pl.when(i > 0)
        def _():
            arrived(x, xb_recv.at[u, way, b - 1])

            def body(c):
                for s in range(2):
                    x[s, :, c] = (mine[s, :, c] + x[s, :, c].astype(F32)).astype(BF16)

            lanes(body)

        send(x, x, xb_send.at[u], xb_recv.at[u, way, b - 1], ahead[way])

    def load_state(u):
        @pl.when(u >= 3)
        def _():
            copied(mv.at[lax.rem(u, 3), :, pl.ds(0, A)], sta.at[lax.rem(u, 3)])
            copied(mv.at[lax.rem(u, 3), :, pl.ds(A, B)], stb.at[lax.rem(u, 3)])

        def go(which, layer, q):
            for i, from_ in enumerate((ms, vs)):
                source = cut(from_[which], which, (layer,), q, 0, ROWS)
                pltpu.make_async_copy(source, mv.at[lax.rem(u, 3), i], mv_load.at[lax.rem(u, 3)]).start()
            for buffer, sem, first, count in ((wa, wa_load, 0, A), (wb, wb_load, A, B)):
                source = cut(weights[which], which, (layer, y, z, core), q, first, count)
                pltpu.make_async_copy(source, buffer.at[u], sem.at[lax.rem(u, 3)]).start()

        each(u, go)

    def adamw(g, w_ref, u, first, count, c):
        rows = pl.ds(first, count)
        m_ref, v_ref = mv.at[lax.rem(u, 3), 0], mv.at[lax.rem(u, 3), 1]
        g = g.astype(BF16).astype(F32)
        w = w_ref[:, c].astype(F32)
        m = 0.9 * m_ref[rows, c] + 0.1 * g
        v = 0.95 * v_ref[rows, c] + 0.05 * g * g
        step = m * lax.rsqrt(v + 1e-8) + 0.1 * w
        w_ref[:, c] = (w - 0.02 * step).astype(BF16)
        m_ref[rows, c] = m
        v_ref[rows, c] = v

    def spread(which, layer, q, u, buffer, first, count, own_sem, st, across_sent, across_received, line_sent, line_received):
        where = cut(new_w[which], which, (layer, y, z, core), q, first, count)
        if line_sent is not None:
            for way in range(2):

                @pl.when(place[way] < 3)
                def _(way=way):
                    send(buffer.at[u], where, line_sent.at[u], line_received(way), ahead[way])

        send(buffer.at[u], where, across_sent.at[u], across_received.at[u], across)
        pltpu.make_async_copy(buffer.at[u], where, own_sem.at[u]).start()
        for i, to in enumerate((new_m, new_v)):
            target = cut(to[which], which, (layer,), q, first, count)
            pltpu.make_async_copy(mv.at[lax.rem(u, 3), i, pl.ds(first, count)], target, st.at[lax.rem(u, 3)]).start()

    def step_a(u):
        copied(wa.at[u], wa_load.at[lax.rem(u, 3)])
        mine = la.at[lax.rem(u, 3), z]
        for way in range(2):

            @pl.when(place[way] > 0)
            def _(way=way):
                x = xa.at[u, way, place[way] - 1]
                arrived(x, xa_recv.at[u, way, place[way] - 1])

                def body(c):
                    mine[:, c] = mine[:, c] + x[:, c].astype(F32)

                lanes(body)

        lanes(lambda c: adamw(mine[:, c], wa.at[u], u, 0, A, c))

        def go(which, layer, q):
            spread(which, layer, q, u, wa, 0, A, own_a, sta, ya_send, ya_recv, ga_send, lambda way: ga_recv.at[u, way, place[way]])

        each(u, go)

    def line_b(u):
        copied(mv.at[lax.rem(u, 3)], mv_load.at[lax.rem(u, 3)])
        mine = lb.at[lax.rem(u, 3), z]
        for way in range(2):

            @pl.when(place[way] > 0)
            def _(way=way):
                x = xb.at[u, way, place[way] - 1]
                arrived(x, xb_recv.at[u, way, place[way] - 1])

                def body(c):
                    for s in range(2):
                        mine[s, :, c] = mine[s, :, c] + x[s, :, c].astype(F32)

                lanes(body)

        def body(c):
            out_z[u, :, c] = mine[1 - y, :, c].astype(BF16)

        lanes(body)
        send(out_z.at[u], in_z.at[u], z_send.at[u], z_recv.at[u], across)

    def step_b(u):
        copied(wb.at[u], wb_load.at[lax.rem(u, 3)])
        arrived(in_z.at[u], z_recv.at[u], across)
        mine = lb.at[lax.rem(u, 3), z]
        lanes(lambda c: adamw(mine[y, :, c] + in_z[u, :, c].astype(F32), wb.at[u], u, A, B, c))

        def go(which, layer, q):
            spread(which, layer, q, u, wb, A, B, own_b, stb, yb_send, yb_recv, gb_send if B_OWN == B_STEP else None, lambda way: gb_recv.at[u, way, place[way], 0])

        each(u, go)

    def relay_a(u, way, b):
        arrived(wa.at[u], ga_recv.at[u, way, b])

        def go(which, layer, q):
            where = cut(new_w[which], which, (layer, y, z_of(way, b), core), q, 0, A)

            @pl.when(place[way] < 3)
            def _():
                send(where, where, ga_send.at[u], ga_recv.at[u, way, b], ahead[way])

            send(where, where, ya_send.at[u], ya_recv.at[u], across)

        each(u, go)

    def relay_b(u, way, b, s):
        arrived(wb.at[u], gb_recv.at[u, way, b, s])

        @pl.when(place[way] < 3)
        def _():
            def go(which, layer, q):
                row = y if s == 0 else 1 - y
                where = cut(new_w[which], which, (layer, row, z_of(way, b), core), q, A, B)
                send(where, where, gb_send.at[u], gb_recv.at[u, way, b, s], ahead[way])

            each(u, go)

    def own_b_out(u):
        def go(which, layer, q):
            where = cut(new_w[which], which, (layer, y, z, core), q, A, B)
            for way in range(2):

                @pl.when(place[way] < 3)
                def _(way=way):
                    send(wb.at[u], where, gb_send.at[u], gb_recv.at[u, way, place[way], 0], ahead[way])

        each(u, go)

    def from_across_b(u):
        arrived(wb.at[u], yb_recv.at[u], across)

        def go(which, layer, q):
            where = cut(new_w[which], which, (layer, 1 - y, z, core), q, A, B)
            for way in range(2):

                @pl.when(place[way] < 3)
                def _(way=way):
                    send(where, where, gb_send.at[u], gb_recv.at[u, way, place[way], 1], ahead[way])

        each(u, go)

    def hand_over(u):
        arrived(out_y.at[u], ya_recv.at[u], across)
        copied(wa.at[u], own_a.at[u])
        copied(wb.at[u], own_b.at[u])

        def go(which, layer, q):
            where = cut(new_w[which], which, (layer, slice(None), slice(None), core), q, 0, ROWS)
            send(where, where, hand_send.at[u], hand_recv.at[u], other)

        each(u, go)

    def when(condition, body, *args):
        @pl.when(condition)
        def _():
            body(*args)

    def hops_a(u, f):
        for way in range(2):
            when(place[way] <= f, hop_a, u, way, 3 - f + place[way])

    def hops_b(u, f):
        for way in range(2):
            when(place[way] <= f, hop_b, u, way, 3 - f + place[way])

    def relays_a(u, k):
        for way in range(2):
            when(place[way] >= k, relay_a, u, way, place[way] - k)

    def relays_b(u, k, s):
        for way in range(2):
            when(place[way] >= k, relay_b, u, way, place[way] - k, s)

    early = [(LAG + f, hops_a, f) for f in range(3)] + [(f, hops_b, f) for f in range(3)]
    early = early[::-1] if B_FIRST else early
    early += [(LAG + 3 + k, relays_a, k) for k in range(1, 4)]
    early += [(LAG + 3, step_a), (3, line_b)]
    middle = [(LAG - 8 + b, sum_t, b) for b in range(4)]
    middle += [(-4, sum_b, 0, 2), (-3, sum_b, 2, 2), (LAG - 2, sum_a, 0, 2), (LAG - 1, sum_a, 2, 2)]
    middle += [(-16, to_partner), (LAG - 9, load_t), (-7, load_b), (LAG - 3, load_a), (1, load_state)]
    late = [(B_OWN + k, relays_b, k, 0) for k in range(1, 4)] + [(B_OTHER + k, relays_b, k, 1) for k in range(1, 4)]
    late += [(B_STEP, step_b)] + ([(B_OWN, own_b_out)] if B_OWN != B_STEP else []) + [(B_OTHER, from_across_b), (HAND, hand_over)]

    to_partner(0)

    def period(r, _):
        for f in range(4):
            for offset, body, *rest in early + middle + late:
                if offset % 4 == f:
                    u = r - offset // 4
                    when(jnp.logical_and(u >= 0, u < UNITS), body, u, *rest)
        return 0

    lax.fori_loop(0, UNITS + 3 + HAND // 4, lambda n, _: period(n - 3, _), 0)

    for u in range(3):
        copied(mv.at[u, :, pl.ds(0, A)], sta.at[u])
        copied(mv.at[u, :, pl.ds(A, B)], stb.at[u])

    def sent(like, sem):
        pltpu.make_async_remote_copy(like, like, sem, sem, device_id=other, device_id_type=MESH).wait_send()

    inner = lax.div(z + 1, 2) == 1

    def drain(u, _):
        sent(partner.at[u], pair_send.at[u])
        sent(out_y.at[u], y_send.at[u])
        sent(out_z.at[u], z_send.at[u])
        sent(xa.at[u, 0], xa_send.at[u])
        sent(xb.at[u, 0], xb_send.at[u])
        sent(out_y.at[u], ya_send.at[u])
        sent(wb.at[u], yb_send.at[u])
        sent(partner.at[u], hand_send.at[u])

        @pl.when(inner)
        def _():
            sent(xa.at[pl.ds(0, 5), 0, 0], ga_send.at[u])
            sent(xb.at[pl.ds(0, 5), 0, 0], gb_send.at[u])

        @pl.when(jnp.logical_not(inner))
        def _():
            sent(xa.at[0, 0, 0], ga_send.at[u])
            sent(xb.at[0, 0, 0], gb_send.at[u])

        arrived(partner.at[u], hand_recv.at[u])
        return 0

    lax.fori_loop(0, UNITS, drain, 0)


def solution(mesh):
    def step(*arrays):
        def split(i, a):
            if i % 3 == 2:
                return a.reshape(2, 2, 4, 2, 4, ROWS, LANES)
            return a.reshape(2, 2, 4, 2, ROWS, 4 * LANES)

        whole = [split(i, a) for i, a in enumerate(arrays[:6])]
        moments = [a if i % 3 < 2 else a.reshape(2, 4, ROWS, LANES) for i, a in enumerate(arrays[6:])]
        dma = pltpu.SemaphoreType.DMA
        by_unit = dma((UNITS,))
        out = pl.pallas_call(
            kernel,
            out_shape=(
                *(jax.ShapeDtypeStruct(a.shape, a.dtype) for a in (*whole[3:], *moments)),
                jax.ShapeDtypeStruct((UNITS, 2, 4, ROWS, LANES), BF16),
                jax.ShapeDtypeStruct((UNITS, 4, A, LANES), BF16),
            ),
            in_specs=[pl.BlockSpec(memory_space=pl.ANY)] * 12,
            out_specs=[pl.BlockSpec(memory_space=pl.ANY)] * 11,
            scratch_shapes=[
                pltpu.VMEM((UNITS, 2, 3, A, LANES), BF16),
                pltpu.VMEM((UNITS, 2, 3, 2, B, LANES), BF16),
                pltpu.VMEM((UNITS, 4, A, LANES), BF16),
                pltpu.VMEM((UNITS, B, LANES), BF16),
                pltpu.VMEM((UNITS, B, LANES), BF16),
                pltpu.VMEM((3, 4, A, LANES), F32),
                pltpu.VMEM((3, 4, 2, B, LANES), F32),
                pltpu.VMEM((2, 4, A, LANES), BF16),
                pltpu.VMEM((3, 4, A, LANES), BF16),
                pltpu.VMEM((2, 2, 4, B, LANES), BF16),
                pltpu.VMEM((UNITS, A, LANES), BF16),
                pltpu.VMEM((UNITS, B, LANES), BF16),
                pltpu.VMEM((3, 2, ROWS, LANES), F32),
                *(by_unit, by_unit),
                *(dma((2,)), dma((3,)), dma((2,)), *(dma((3,)),) * 5, by_unit, by_unit),
                *(by_unit,) * 4,
                *(by_unit, dma((UNITS, 2, 3)), by_unit, dma((UNITS, 2, 3))),
                *(by_unit, dma((UNITS, 2, 3)), by_unit, dma((UNITS, 2, 3, 2))),
                *(by_unit,) * 6,
            ],
            compiler_params=pltpu.CompilerParams(collective_id=0, has_side_effects=True, vmem_limit_bytes=62 * 1024 * 1024),
        )(*whole, *moments)
        return tuple(a.reshape(like.shape) for a, like in zip(out[:9], arrays[3:], strict=True))

    all_of, cut = P(None, None, None), P(None, "dp", None)
    return jax.shard_map(
        step,
        mesh=mesh,
        in_specs=(P(("rep", "dp"), None, None, None),) * 3 + (all_of,) * 3 + (cut,) * 6,
        out_specs=(P("rep", None, None),) * 3 + (P("rep", "dp", None),) * 6,
        check_vma=False,
    )
```

```python
import jax
import jax.numpy as jnp
from jax import lax
from jax.experimental import pallas as pl
from jax.experimental.pallas import tpu as pltpu
from jax.sharding import PartitionSpec as P

F32, BF16 = jnp.float32, jnp.bfloat16
MESH = pl.DeviceIdType.MESH
UNITS = 24
RING, SLOTS = 4, 5
ROWS, A, B, LANES = 72, 40, 32, 1152
LAG, B_STEP, B_OWN, B_OTHER, HAND, B_FIRST = 2, 4, 4, 5, 10, False


def lanes(body):
    def at(j, _):
        body(pl.ds(pl.multiple_of(j * 384, 384), 384))
        return 0

    lax.fori_loop(0, 3, at, 0)


def kernel(*refs):
    terms, weights, ms, vs = (refs[i : i + 3] for i in (0, 3, 6, 9))
    new_w = refs[12:15]
    mv, partner, over_y = refs[15:18]
    xa, xb, out_y, out_z, in_z, la, lb, t_in, a_in, b_in, wa, wb = refs[18:30]
    (
        pair_send, pair_recv, t_load, a_load, b_load, mv_load, wa_load, wb_load, own_a, own_b,
        y_send, y_recv, z_send, z_recv, xa_send, xa_recv, xb_send, xb_recv,
        ga_send, ga_recv, gb_send, gb_recv, ya_send, ya_recv, yb_send, yb_recv, hand_send, hand_recv,
    ) = refs[30:]

    me = lax.axis_index("dp")
    core = lax.rem(me, 2)
    z = lax.rem(lax.div(me, 2), 4)
    y = lax.div(me, 8)
    other = {"dp": me + 1 - 2 * core}
    across = {"dp": me + 8 - 16 * y}
    ahead = ({"dp": me + 2}, {"dp": me - 2})
    place = (z, 3 - z)

    barrier = pltpu.get_barrier_semaphore()
    for device in (other, across):
        pl.semaphore_signal(barrier, inc=1, device_id=device, device_id_type=MESH)
    for way in range(2):

        @pl.when(place[way] < 3)
        def _(way=way):
            pl.semaphore_signal(barrier, inc=1, device_id=ahead[way], device_id_type=MESH)

    pl.semaphore_wait(barrier, 2 + lax.div(z + 2, 3) + lax.div(5 - z, 3))

    def z_of(way, b):
        return b if way == 0 else 3 - b

    def each(u, body):
        for which in range(3):

            @pl.when(lax.div(u, 8) == which)
            def _(which=which):
                body(which, lax.rem(lax.div(u, 4), 2), lax.rem(u, 4))

    def cut(ref, which, lead, q, first, count):
        if which == 2:
            return ref.at[(*lead, q, pl.ds(first, count))]
        return ref.at[(*lead, pl.ds(first, count), pl.ds(pl.multiple_of(q * LANES, 128), LANES))]

    def send(source, target, sent, received, device):
        pltpu.make_async_remote_copy(source, target, sent, received, device_id=device, device_id_type=MESH).start()

    def arrived(like, sem, device=other):
        pltpu.make_async_remote_copy(like, like, sem, sem, device_id=device, device_id_type=MESH).wait_recv()

    def copied(like, sem):
        pltpu.make_async_copy(like, like, sem).wait()

    def to_partner(u):
        def go(which, layer, q):
            source = cut(terms[which], which, (layer, slice(None), slice(None), 1 - core), q, 0, ROWS)
            send(source, partner.at[u], pair_send.at[u], pair_recv.at[u], other)

        each(u, go)

    def load_t(u):
        arrived(partner.at[u], pair_recv.at[u])

        def go(which, layer, q):
            source = cut(terms[which], which, (layer, 1 - y, slice(None), core), q, 0, A)
            pltpu.make_async_copy(source, t_in.at[0], t_load.at[0]).start()

        each(u, go)
        pltpu.make_async_copy(partner.at[u, 1 - y, :, pl.ds(0, A)], t_in.at[1], t_load.at[1]).start()

    def sum_t(u, b):
        if b == 0:
            for i in range(2):
                copied(t_in.at[i], t_load.at[i])

        def body(c):
            out_y[lax.rem(u, RING), b, :, c] = (t_in[0, b, :, c].astype(F32) + t_in[1, b, :, c].astype(F32)).astype(BF16)

        lanes(body)
        send(out_y.at[lax.rem(u, RING), b], over_y.at[u, b], y_send.at[u], y_recv.at[u], across)

    def load_a(u):
        arrived(over_y.at[u], y_recv.at[u], across)

        def go(which, layer, q):
            source = cut(terms[which], which, (layer, y, slice(None), core), q, 0, A)
            pltpu.make_async_copy(source, a_in.at[0], a_load.at[0]).start()

        each(u, go)
        pltpu.make_async_copy(partner.at[u, y, :, pl.ds(0, A)], a_in.at[1], a_load.at[1]).start()
        pltpu.make_async_copy(over_y.at[u], a_in.at[2], a_load.at[2]).start()

    def sum_a(u, first, count):
        if first == 0:
            for i in range(3):
                copied(a_in.at[i], a_load.at[i])

        def one(b, _):
            def body(c):
                la[lax.rem(u, 3), b, :, c] = (
                    a_in[0, b, :, c].astype(F32) + a_in[1, b, :, c].astype(F32) + a_in[2, b, :, c].astype(F32)
                )

            lanes(body)
            return 0

        lax.fori_loop(first, first + count, one, 0)

    def load_b(u):
        def go(which, layer, q):
            source = cut(terms[which], which, (layer, slice(None), slice(None), core), q, A, B)
            pltpu.make_async_copy(source, b_in.at[0], b_load.at[0]).start()

        each(u, go)
        pltpu.make_async_copy(partner.at[u, :, :, pl.ds(A, B)], b_in.at[1], b_load.at[1]).start()

    def sum_b(u, first, count):
        if first == 0:
            for i in range(2):
                copied(b_in.at[i], b_load.at[i])

        def one(n, _):
            b, s = lax.div(n, 2), lax.rem(n, 2)

            def body(c):
                lb[lax.rem(u, 3), b, s, :, c] = b_in[0, s, b, :, c].astype(F32) + b_in[1, s, b, :, c].astype(F32)

            lanes(body)
            return 0

        lax.fori_loop(2 * first, 2 * (first + count), one, 0)

    def hop_a(u, way, b):
        i = place[way]
        x = xa.at[lax.rem(u, RING), way, b - 1]
        mine = la.at[lax.rem(u, 3), z_of(way, b)]

        @pl.when(i == 0)
        def _():
            def body(c):
                x[:, c] = mine[:, c].astype(BF16)

            lanes(body)

        @pl.when(i > 0)
        def _():
            arrived(x, xa_recv.at[u, way, b - 1])

            def body(c):
                x[:, c] = (mine[:, c] + x[:, c].astype(F32)).astype(BF16)

            lanes(body)

        send(x, x, xa_send.at[u], xa_recv.at[u, way, b - 1], ahead[way])

    def hop_b(u, way, b):
        i = place[way]
        x = xb.at[lax.rem(u, RING), way, b - 1]
        mine = lb.at[lax.rem(u, 3), z_of(way, b)]

        @pl.when(i == 0)
        def _():
            def body(c):
                for s in range(2):
                    x[s, :, c] = mine[s, :, c].astype(BF16)

            lanes(body)

        @pl.when(i > 0)
        def _():
            arrived(x, xb_recv.at[u, way, b - 1])

            def body(c):
                for s in range(2):
                    x[s, :, c] = (mine[s, :, c] + x[s, :, c].astype(F32)).astype(BF16)

            lanes(body)

        send(x, x, xb_send.at[u], xb_recv.at[u, way, b - 1], ahead[way])

    def load_state(u):
        def go(which, layer, q):
            for i, from_ in enumerate((ms, vs)):
                source = cut(from_[which], which, (layer,), q, 0, ROWS)
                pltpu.make_async_copy(source, mv.at[u, i], mv_load.at[lax.rem(u, 3)]).start()
            for buffer, sem, first, count in ((wa, wa_load, 0, A), (wb, wb_load, A, B)):
                source = cut(weights[which], which, (layer, y, z, core), q, first, count)
                pltpu.make_async_copy(source, buffer.at[u], sem.at[lax.rem(u, 3)]).start()

        each(u, go)

    def adamw(g, w_ref, u, first, count, c):
        rows = pl.ds(first, count)
        m_ref, v_ref = mv.at[u, 0], mv.at[u, 1]
        g = g.astype(BF16).astype(F32)
        w = w_ref[:, c].astype(F32)
        m = 0.9 * m_ref[rows, c] + 0.1 * g
        v = 0.95 * v_ref[rows, c] + 0.05 * g * g
        step = m * lax.rsqrt(v + 1e-8) + 0.1 * w
        w_ref[:, c] = (w - 0.02 * step).astype(BF16)
        m_ref[rows, c] = m
        v_ref[rows, c] = v

    def spread(which, layer, q, u, buffer, first, count, own_sem, across_sent, across_received, line_sent, line_received):
        where = cut(new_w[which], which, (layer, y, z, core), q, first, count)
        if line_sent is not None:
            for way in range(2):

                @pl.when(place[way] < 3)
                def _(way=way):
                    send(buffer.at[u], where, line_sent.at[u], line_received(way), ahead[way])

        send(buffer.at[u], where, across_sent.at[u], across_received.at[u], across)
        pltpu.make_async_copy(buffer.at[u], where, own_sem.at[u]).start()

    def step_a(u):
        copied(wa.at[u], wa_load.at[lax.rem(u, 3)])
        mine = la.at[lax.rem(u, 3), z]
        for way in range(2):

            @pl.when(place[way] > 0)
            def _(way=way):
                x = xa.at[lax.rem(u, RING), way, place[way] - 1]
                arrived(x, xa_recv.at[u, way, place[way] - 1])

                def body(c):
                    mine[:, c] = mine[:, c] + x[:, c].astype(F32)

                lanes(body)

        lanes(lambda c: adamw(mine[:, c], wa.at[u], u, 0, A, c))

        def go(which, layer, q):
            spread(which, layer, q, u, wa, 0, A, own_a, ya_send, ya_recv, ga_send, lambda way: ga_recv.at[u, way, place[way]])

        each(u, go)

    def line_b(u):
        copied(mv.at[u], mv_load.at[lax.rem(u, 3)])
        mine = lb.at[lax.rem(u, 3), z]
        for way in range(2):

            @pl.when(place[way] > 0)
            def _(way=way):
                x = xb.at[lax.rem(u, RING), way, place[way] - 1]
                arrived(x, xb_recv.at[u, way, place[way] - 1])

                def body(c):
                    for s in range(2):
                        mine[s, :, c] = mine[s, :, c] + x[s, :, c].astype(F32)

                lanes(body)

        def body(c):
            out_z[u, :, c] = mine[1 - y, :, c].astype(BF16)

        lanes(body)
        send(out_z.at[u], in_z.at[u], z_send.at[u], z_recv.at[u], across)

    def step_b(u):
        copied(wb.at[u], wb_load.at[lax.rem(u, 3)])
        arrived(in_z.at[u], z_recv.at[u], across)
        mine = lb.at[lax.rem(u, 3), z]
        lanes(lambda c: adamw(mine[y, :, c] + in_z[u, :, c].astype(F32), wb.at[u], u, A, B, c))

        def go(which, layer, q):
            spread(which, layer, q, u, wb, A, B, own_b, yb_send, yb_recv, gb_send if B_OWN == B_STEP else None, lambda way: gb_recv.at[u, way, place[way], 0])

        each(u, go)

    def relay_a(u, way, b):
        arrived(wa.at[u], ga_recv.at[u, way, b])

        def go(which, layer, q):
            where = cut(new_w[which], which, (layer, y, z_of(way, b), core), q, 0, A)

            @pl.when(place[way] < 3)
            def _():
                send(where, where, ga_send.at[u], ga_recv.at[u, way, b], ahead[way])

            send(where, where, ya_send.at[u], ya_recv.at[u], across)

        each(u, go)

    def relay_b(u, way, b, s):
        arrived(wb.at[u], gb_recv.at[u, way, b, s])

        @pl.when(place[way] < 3)
        def _():
            def go(which, layer, q):
                row = y if s == 0 else 1 - y
                where = cut(new_w[which], which, (layer, row, z_of(way, b), core), q, A, B)
                send(where, where, gb_send.at[u], gb_recv.at[u, way, b, s], ahead[way])

            each(u, go)

    def own_b_out(u):
        def go(which, layer, q):
            where = cut(new_w[which], which, (layer, y, z, core), q, A, B)
            for way in range(2):

                @pl.when(place[way] < 3)
                def _(way=way):
                    send(wb.at[u], where, gb_send.at[u], gb_recv.at[u, way, place[way], 0], ahead[way])

        each(u, go)

    def from_across_b(u):
        arrived(wb.at[u], yb_recv.at[u], across)

        def go(which, layer, q):
            where = cut(new_w[which], which, (layer, 1 - y, z, core), q, A, B)
            for way in range(2):

                @pl.when(place[way] < 3)
                def _(way=way):
                    send(where, where, gb_send.at[u], gb_recv.at[u, way, place[way], 1], ahead[way])

        each(u, go)

    def hand_over(u):
        arrived(out_y.at[0], ya_recv.at[u], across)
        copied(wa.at[u], own_a.at[u])
        copied(wb.at[u], own_b.at[u])

        def go(which, layer, q):
            where = cut(new_w[which], which, (layer, slice(None), slice(None), core), q, 0, ROWS)
            send(where, where, hand_send.at[u], hand_recv.at[u], other)

        each(u, go)

    def when(condition, body, *args):
        @pl.when(condition)
        def _():
            body(*args)

    def hops_a(u, f):
        for way in range(2):
            when(place[way] <= f, hop_a, u, way, 3 - f + place[way])

    def hops_b(u, f):
        for way in range(2):
            when(place[way] <= f, hop_b, u, way, 3 - f + place[way])

    def relays_a(u, k):
        for way in range(2):
            when(place[way] >= k, relay_a, u, way, place[way] - k)

    def relays_b(u, k, s):
        for way in range(2):
            when(place[way] >= k, relay_b, u, way, place[way] - k, s)

    def sent(like, sem):
        pltpu.make_async_remote_copy(like, like, sem, sem, device_id=other, device_id_type=MESH).wait_send()

    def free_x(u):
        sent(xa.at[0, 0], xa_send.at[u])
        sent(xb.at[0, 0], xb_send.at[u])

    def free_y(u):
        sent(out_y.at[0], y_send.at[u])

    early = [(LAG + f, hops_a, f) for f in range(3)] + [(f, hops_b, f) for f in range(3)]
    early = early[::-1] if B_FIRST else early
    early += [(LAG + 3 + k, relays_a, k) for k in range(1, 4)]
    early += [(LAG + 3, step_a), (3, line_b)]
    middle = [(LAG - 8 + b, sum_t, b) for b in range(4)]
    middle += [(-4, sum_b, 0, 2), (-3, sum_b, 2, 2), (LAG - 1, sum_a, 0, 4)]
    middle += [(-16, to_partner), (LAG - 9, load_t), (-7, load_b), (LAG - 2, load_a), (1, load_state), (8, free_x), (3, free_y)]
    late = [(B_OWN + k, relays_b, k, 0) for k in range(1, 4)] + [(B_OTHER + k, relays_b, k, 1) for k in range(1, 4)]
    late += [(B_STEP, step_b)] + ([(B_OWN, own_b_out)] if B_OWN != B_STEP else []) + [(B_OTHER, from_across_b), (HAND, hand_over)]

    to_partner(0)

    def period(r, _):
        for f in range(4):
            for offset, body, *rest in early + middle + late:
                if offset % 4 == f:
                    u = r - offset // 4
                    when(jnp.logical_and(u >= 0, u < UNITS), body, u, *rest)
        return 0

    lax.fori_loop(0, UNITS + 3 + HAND // 4, lambda n, _: period(n - 3, _), 0)

    inner = lax.div(z + 1, 2) == 1

    def drain(u, _):
        sent(partner.at[u], pair_send.at[u])
        sent(out_z.at[u], z_send.at[u])
        sent(out_y.at[0], ya_send.at[u])
        sent(wb.at[u], yb_send.at[u])
        sent(partner.at[u], hand_send.at[u])

        @pl.when(inner)
        def _():
            sent(wa.at[pl.ds(0, 5)], ga_send.at[u])
            sent(wb.at[pl.ds(0, 10)], gb_send.at[u])

        @pl.when(jnp.logical_not(inner))
        def _():
            sent(wa.at[0], ga_send.at[u])
            sent(wb.at[pl.ds(0, 2)], gb_send.at[u])

        arrived(partner.at[u], hand_recv.at[u])
        return 0

    lax.fori_loop(0, UNITS, drain, 0)


def unload(gate, up, down, mv, *refs):
    new_w, new_m, new_v = refs[:3], refs[3:6], refs[6:9]
    slots, in_sem, out_sem, down_sem, mv_sem = refs[9:]
    chunks = [(which, layer, row, half) for which in range(2) for layer in range(2) for row in range(2) for half in range(2)]
    sources = (gate, up, down)

    def read(n):
        which, layer, row, half = chunks[n]
        return pltpu.make_async_copy(sources[which].at[layer, row, pl.ds(2 * half, 2)], slots.at[n % SLOTS], in_sem.at[n % SLOTS])

    def write(n):
        which, layer, row, half = chunks[n]
        return pltpu.make_async_copy(slots.at[n % SLOTS], new_w[which].at[layer, row, pl.ds(2 * half, 2)], out_sem.at[n % SLOTS])

    for n in range(SLOTS):
        read(n).start()
    pltpu.make_async_copy(down, new_w[2], down_sem).start()
    for u in range(UNITS):
        which, layer, q = u // 8, u // 4 % 2, u % 4
        for i, to in enumerate((new_m, new_v)):
            target = to[which].at[layer, q] if which == 2 else to[which].at[layer, :, pl.ds(q * LANES, LANES)]
            pltpu.make_async_copy(mv.at[u, i], target, mv_sem).start()
    for n in range(len(chunks)):
        read(n).wait()
        write(n).start()
        ahead = n + SLOTS - 2
        if n >= 2 and ahead < len(chunks):
            write(ahead - SLOTS).wait()
            read(ahead).start()
    for n in range(len(chunks) - SLOTS, len(chunks)):
        write(n).wait()
    pltpu.make_async_copy(down, down, down_sem).wait()
    pltpu.make_async_copy(mv, mv, mv_sem).wait()


def solution(mesh):
    def step(*arrays):
        def split(i, a):
            if i % 3 == 2:
                return a.reshape(2, 2, 4, 2, 4, ROWS, LANES)
            return a.reshape(2, 2, 4, 2, ROWS, 4 * LANES)

        whole = [split(i, a) for i, a in enumerate(arrays[:6])]
        moments = [a if i % 3 < 2 else a.reshape(2, 4, ROWS, LANES) for i, a in enumerate(arrays[6:])]
        dma = pltpu.SemaphoreType.DMA
        by_unit = dma((UNITS,))
        hbm = [jax.ShapeDtypeStruct(a.shape, a.dtype) for a in whole[3:]]
        kept = [pltpu.VMEM(whole[5].shape, BF16), pltpu.VMEM((UNITS, 2, ROWS, LANES), F32)]
        out = pl.pallas_call(
            kernel,
            out_shape=(
                *hbm[:2],
                *kept,
                jax.ShapeDtypeStruct((UNITS, 2, 4, ROWS, LANES), BF16),
                jax.ShapeDtypeStruct((UNITS, 4, A, LANES), BF16),
            ),
            in_specs=[pl.BlockSpec(memory_space=pl.ANY)] * 12,
            out_specs=[pl.BlockSpec(memory_space=space) for space in (pl.ANY, pl.ANY, pltpu.VMEM, pltpu.VMEM, pl.ANY, pl.ANY)],
            scratch_shapes=[
                pltpu.VMEM((RING, 2, 3, A, LANES), BF16),
                pltpu.VMEM((RING, 2, 3, 2, B, LANES), BF16),
                pltpu.VMEM((RING, 4, A, LANES), BF16),
                pltpu.VMEM((UNITS, B, LANES), BF16),
                pltpu.VMEM((UNITS, B, LANES), BF16),
                pltpu.VMEM((3, 4, A, LANES), F32),
                pltpu.VMEM((3, 4, 2, B, LANES), F32),
                pltpu.VMEM((2, 4, A, LANES), BF16),
                pltpu.VMEM((3, 4, A, LANES), BF16),
                pltpu.VMEM((2, 2, 4, B, LANES), BF16),
                pltpu.VMEM((UNITS, A, LANES), BF16),
                pltpu.VMEM((UNITS, B, LANES), BF16),
                *(by_unit, by_unit),
                *(dma((2,)), dma((3,)), dma((2,)), *(dma((3,)),) * 3, by_unit, by_unit),
                *(by_unit,) * 4,
                *(by_unit, dma((UNITS, 2, 3)), by_unit, dma((UNITS, 2, 3))),
                *(by_unit, dma((UNITS, 2, 3)), by_unit, dma((UNITS, 2, 3, 2))),
                *(by_unit,) * 6,
            ],
            compiler_params=pltpu.CompilerParams(collective_id=0, has_side_effects=True, vmem_limit_bytes=24 * 1024 * 1024),
        )(*whole, *moments)
        final = pl.pallas_call(
            unload,
            out_shape=(*hbm, *(jax.ShapeDtypeStruct(a.shape, a.dtype) for a in moments)),
            in_specs=[pl.BlockSpec(memory_space=space) for space in (pltpu.HBM, pltpu.HBM, pltpu.VMEM, pltpu.VMEM)],
            out_specs=[pl.BlockSpec(memory_space=pl.ANY)] * 9,
            scratch_shapes=[pltpu.VMEM((SLOTS, 2, 2, ROWS, 4 * LANES), BF16), dma((SLOTS,)), dma((SLOTS,)), dma, dma],
            compiler_params=pltpu.CompilerParams(vmem_limit_bytes=24 * 1024 * 1024),
        )(*(pltpu.with_memory_space_constraint(a, space) for a, space in zip(out[:4], (pltpu.HBM, pltpu.HBM, pltpu.VMEM, pltpu.VMEM), strict=True)))
        return tuple(a.reshape(like.shape) for a, like in zip(final, arrays[3:], strict=True))

    all_of, cut = P(None, None, None), P(None, "dp", None)
    return jax.shard_map(
        step,
        mesh=mesh,
        in_specs=(P(("rep", "dp"), None, None, None),) * 3 + (all_of,) * 3 + (cut,) * 6,
        out_specs=(P("rep", None, None),) * 3 + (P("rep", "dp", None),) * 6,
        check_vma=False,
    )
```

```python
import jax
import jax.numpy as jnp
from jax import lax
from jax.experimental import pallas as pl
from jax.experimental.pallas import tpu as pltpu
from jax.sharding import PartitionSpec as P

F32, BF16 = jnp.float32, jnp.bfloat16
MESH = pl.DeviceIdType.MESH
UNITS = 24
RING, SLOTS = 4, 5
ROWS, A, B, LANES = 72, 40, 32, 1152
GA, GB = 48, 24
LAG, B_STEP, B_OWN, B_OTHER, HAND, B_FIRST = 2, 4, 4, 5, 10, False


def lanes(body):
    def at(j, _):
        body(pl.ds(pl.multiple_of(j * 384, 384), 384))
        return 0

    lax.fori_loop(0, 3, at, 0)


def kernel(*refs):
    terms, weights, ms, vs = (refs[i : i + 3] for i in (0, 3, 6, 9))
    new_w = refs[12:15]
    mv, partner, over_y = refs[15:18]
    xa, xb, out_y, out_z, in_z, la, lb, t_in, a_in, b_in, w_own = refs[18:29]
    (
        pair_send, pair_recv, t_load, a_load, b_load, mv_load, w_load, own_a, own_b,
        y_send, y_recv, z_send, z_recv, xa_send, xa_recv, xb_send, xb_recv,
        ga_send, ga_recv, gb_send, gb_recv, ya_send, ya_recv, yb_send, yb_recv, hand_send, hand_recv,
    ) = refs[29:]

    me = lax.axis_index("dp")
    core = lax.rem(me, 2)
    z = lax.rem(lax.div(me, 2), 4)
    y = lax.div(me, 8)
    other = {"dp": me + 1 - 2 * core}
    across = {"dp": me + 8 - 16 * y}
    ahead = ({"dp": me + 2}, {"dp": me - 2})
    place = (z, 3 - z)

    barrier = pltpu.get_barrier_semaphore()
    for device in (other, across):
        pl.semaphore_signal(barrier, inc=1, device_id=device, device_id_type=MESH)
    for way in range(2):

        @pl.when(place[way] < 3)
        def _(way=way):
            pl.semaphore_signal(barrier, inc=1, device_id=ahead[way], device_id_type=MESH)

    pl.semaphore_wait(barrier, 2 + lax.div(z + 2, 3) + lax.div(5 - z, 3))

    def z_of(way, b):
        return b if way == 0 else 3 - b

    def each(u, body):
        for which in range(3):

            @pl.when(lax.div(u, 8) == which)
            def _(which=which):
                body(which, lax.rem(lax.div(u, 4), 2), lax.rem(u, 4))

    def cut(ref, which, lead, q, first, count):
        if which == 2:
            return ref.at[(*lead, q, pl.ds(first, count))]
        return ref.at[(*lead, pl.ds(first, count), pl.ds(pl.multiple_of(q * LANES, 128), LANES))]

    def send(source, target, sent, received, device):
        pltpu.make_async_remote_copy(source, target, sent, received, device_id=device, device_id_type=MESH).start()

    def arrived(like, sem, device=other):
        pltpu.make_async_remote_copy(like, like, sem, sem, device_id=device, device_id_type=MESH).wait_recv()

    def copied(like, sem):
        pltpu.make_async_copy(like, like, sem).wait()

    def to_partner(u):
        def go(which, layer, q):
            source = cut(terms[which], which, (layer, slice(None), slice(None), 1 - core), q, 0, ROWS)
            send(source, partner.at[u], pair_send.at[u], pair_recv.at[u], other)

        each(u, go)

    def load_t(u):
        arrived(partner.at[u], pair_recv.at[u])

        def go(which, layer, q):
            source = cut(terms[which], which, (layer, 1 - y, slice(None), core), q, 0, A)
            pltpu.make_async_copy(source, t_in.at[0], t_load.at[0]).start()

        each(u, go)
        pltpu.make_async_copy(partner.at[u, 1 - y, :, pl.ds(0, A)], t_in.at[1], t_load.at[1]).start()

    def sum_t(u, b):
        if b == 0:
            for i in range(2):
                copied(t_in.at[i], t_load.at[i])

        def body(c):
            out_y[lax.rem(u, RING), b, :, c] = (t_in[0, b, :, c].astype(F32) + t_in[1, b, :, c].astype(F32)).astype(BF16)

        lanes(body)
        send(out_y.at[lax.rem(u, RING), b], over_y.at[u, b], y_send.at[u], y_recv.at[u], across)

    def load_a(u):
        arrived(over_y.at[u], y_recv.at[u], across)

        def go(which, layer, q):
            source = cut(terms[which], which, (layer, y, slice(None), core), q, 0, A)
            pltpu.make_async_copy(source, a_in.at[0], a_load.at[0]).start()

        each(u, go)
        pltpu.make_async_copy(partner.at[u, y, :, pl.ds(0, A)], a_in.at[1], a_load.at[1]).start()
        pltpu.make_async_copy(over_y.at[u], a_in.at[2], a_load.at[2]).start()

    def sum_a(u, first, count):
        if first == 0:
            for i in range(3):
                copied(a_in.at[i], a_load.at[i])

        def one(b, _):
            def body(c):
                la[lax.rem(u, 3), b, :, c] = (
                    a_in[0, b, :, c].astype(F32) + a_in[1, b, :, c].astype(F32) + a_in[2, b, :, c].astype(F32)
                )

            lanes(body)
            return 0

        lax.fori_loop(first, first + count, one, 0)

    def load_b(u):
        def go(which, layer, q):
            source = cut(terms[which], which, (layer, slice(None), slice(None), core), q, A, B)
            pltpu.make_async_copy(source, b_in.at[0], b_load.at[0]).start()

        each(u, go)
        pltpu.make_async_copy(partner.at[u, :, :, pl.ds(A, B)], b_in.at[1], b_load.at[1]).start()

    def sum_b(u, first, count):
        if first == 0:
            for i in range(2):
                copied(b_in.at[i], b_load.at[i])

        def one(n, _):
            b, s = lax.div(n, 2), lax.rem(n, 2)

            def body(c):
                lb[lax.rem(u, 3), b, s, :, c] = b_in[0, s, b, :, c].astype(F32) + b_in[1, s, b, :, c].astype(F32)

            lanes(body)
            return 0

        lax.fori_loop(2 * first, 2 * (first + count), one, 0)

    def hop_a(u, way, b):
        i = place[way]
        x = xa.at[lax.rem(u, RING), way, b - 1]
        mine = la.at[lax.rem(u, 3), z_of(way, b)]

        @pl.when(i == 0)
        def _():
            def body(c):
                x[:, c] = mine[:, c].astype(BF16)

            lanes(body)

        @pl.when(i > 0)
        def _():
            arrived(x, xa_recv.at[u, way, b - 1])

            def body(c):
                x[:, c] = (mine[:, c] + x[:, c].astype(F32)).astype(BF16)

            lanes(body)

        send(x, x, xa_send.at[u], xa_recv.at[u, way, b - 1], ahead[way])

    def hop_b(u, way, b):
        i = place[way]
        x = xb.at[lax.rem(u, RING), way, b - 1]
        mine = lb.at[lax.rem(u, 3), z_of(way, b)]

        @pl.when(i == 0)
        def _():
            def body(c):
                for s in range(2):
                    x[s, :, c] = mine[s, :, c].astype(BF16)

            lanes(body)

        @pl.when(i > 0)
        def _():
            arrived(x, xb_recv.at[u, way, b - 1])

            def body(c):
                for s in range(2):
                    x[s, :, c] = (mine[s, :, c] + x[s, :, c].astype(F32)).astype(BF16)

            lanes(body)

        send(x, x, xb_send.at[u], xb_recv.at[u, way, b - 1], ahead[way])

    def load_state(u):
        def go(which, layer, q):
            for i, from_ in enumerate((ms, vs)):
                source = cut(from_[which], which, (layer,), q, 0, ROWS)
                pltpu.make_async_copy(source, mv.at[u, i], mv_load.at[lax.rem(u, 3)]).start()
            source = cut(weights[which], which, (layer, y, z, core), q, 0, ROWS)
            pltpu.make_async_copy(source, w_own.at[u], w_load.at[lax.rem(u, 3)]).start()

        each(u, go)

    def adamw(g, u, first, count, c):
        rows = pl.ds(first, count)
        w_ref, m_ref, v_ref = w_own.at[u], mv.at[u, 0], mv.at[u, 1]
        g = g.astype(BF16).astype(F32)
        w = w_ref[rows, c].astype(F32)
        m = 0.9 * m_ref[rows, c] + 0.1 * g
        v = 0.95 * v_ref[rows, c] + 0.05 * g * g
        step = m * lax.rsqrt(v + 1e-8) + 0.1 * w
        w_ref[rows, c] = (w - 0.02 * step).astype(BF16)
        m_ref[rows, c] = m
        v_ref[rows, c] = v

    def spread(which, layer, q, u, first, count, own_sem, across_sent, across_received, line_sent, line_received):
        where = cut(new_w[which], which, (layer, y, z, core), q, first, count)
        source = w_own.at[u, pl.ds(first, count)]
        if line_sent is not None:
            for way in range(2):

                @pl.when(place[way] < 3)
                def _(way=way):
                    send(source, where, line_sent.at[u], line_received(way), ahead[way])

        send(source, where, across_sent.at[u], across_received.at[u], across)
        pltpu.make_async_copy(source, where, own_sem.at[u]).start()

    def step_a(u):
        mine = la.at[lax.rem(u, 3), z]
        for way in range(2):

            @pl.when(place[way] > 0)
            def _(way=way):
                x = xa.at[lax.rem(u, RING), way, place[way] - 1]
                arrived(x, xa_recv.at[u, way, place[way] - 1])

                def body(c):
                    mine[:, c] = mine[:, c] + x[:, c].astype(F32)

                lanes(body)

        lanes(lambda c: adamw(mine[:, c], u, 0, A, c))

        def go(which, layer, q):
            spread(which, layer, q, u, 0, GA, own_a, ya_send, ya_recv, ga_send, lambda way: ga_recv.at[u, way, place[way]])

        each(u, go)

    def line_b(u):
        copied(mv.at[u], mv_load.at[lax.rem(u, 3)])
        copied(w_own.at[u], w_load.at[lax.rem(u, 3)])
        mine = lb.at[lax.rem(u, 3), z]
        for way in range(2):

            @pl.when(place[way] > 0)
            def _(way=way):
                x = xb.at[lax.rem(u, RING), way, place[way] - 1]
                arrived(x, xb_recv.at[u, way, place[way] - 1])

                def body(c):
                    for s in range(2):
                        mine[s, :, c] = mine[s, :, c] + x[s, :, c].astype(F32)

                lanes(body)

        def body(c):
            out_z[u, :, c] = mine[1 - y, :, c].astype(BF16)

        lanes(body)
        send(out_z.at[u], in_z.at[u], z_send.at[u], z_recv.at[u], across)

    def step_b(u):
        arrived(in_z.at[u], z_recv.at[u], across)
        mine = lb.at[lax.rem(u, 3), z]
        lanes(lambda c: adamw(mine[y, :, c] + in_z[u, :, c].astype(F32), u, A, B, c))

        def go(which, layer, q):
            spread(which, layer, q, u, GA, GB, own_b, yb_send, yb_recv, gb_send if B_OWN == B_STEP else None, lambda way: gb_recv.at[u, way, place[way], 0])

        each(u, go)

    def relay_a(u, way, b):
        arrived(w_own.at[u, pl.ds(0, GA)], ga_recv.at[u, way, b])

        def go(which, layer, q):
            where = cut(new_w[which], which, (layer, y, z_of(way, b), core), q, 0, GA)

            @pl.when(place[way] < 3)
            def _():
                send(where, where, ga_send.at[u], ga_recv.at[u, way, b], ahead[way])

            send(where, where, ya_send.at[u], ya_recv.at[u], across)

        each(u, go)

    def relay_b(u, way, b, s):
        arrived(w_own.at[u, pl.ds(GA, GB)], gb_recv.at[u, way, b, s])

        @pl.when(place[way] < 3)
        def _():
            def go(which, layer, q):
                row = y if s == 0 else 1 - y
                where = cut(new_w[which], which, (layer, row, z_of(way, b), core), q, GA, GB)
                send(where, where, gb_send.at[u], gb_recv.at[u, way, b, s], ahead[way])

            each(u, go)

    def own_b_out(u):
        def go(which, layer, q):
            where = cut(new_w[which], which, (layer, y, z, core), q, GA, GB)
            for way in range(2):

                @pl.when(place[way] < 3)
                def _(way=way):
                    send(w_own.at[u, pl.ds(GA, GB)], where, gb_send.at[u], gb_recv.at[u, way, place[way], 0], ahead[way])

        each(u, go)

    def from_across_b(u):
        arrived(w_own.at[u, pl.ds(GA, GB)], yb_recv.at[u], across)

        def go(which, layer, q):
            where = cut(new_w[which], which, (layer, 1 - y, z, core), q, GA, GB)
            for way in range(2):

                @pl.when(place[way] < 3)
                def _(way=way):
                    send(where, where, gb_send.at[u], gb_recv.at[u, way, place[way], 1], ahead[way])

        each(u, go)

    def hand_over(u):
        arrived(w_own.at[pl.ds(0, 4), pl.ds(0, GA)], ya_recv.at[u], across)
        copied(w_own.at[u, pl.ds(0, GA)], own_a.at[u])
        copied(w_own.at[u, pl.ds(GA, GB)], own_b.at[u])

        def go(which, layer, q):
            where = cut(new_w[which], which, (layer, slice(None), slice(None), core), q, 0, ROWS)
            send(where, where, hand_send.at[u], hand_recv.at[u], other)

        each(u, go)

    def when(condition, body, *args):
        @pl.when(condition)
        def _():
            body(*args)

    def hops_a(u, f):
        for way in range(2):
            when(place[way] <= f, hop_a, u, way, 3 - f + place[way])

    def hops_b(u, f):
        for way in range(2):
            when(place[way] <= f, hop_b, u, way, 3 - f + place[way])

    def relays_a(u, k):
        for way in range(2):
            when(place[way] >= k, relay_a, u, way, place[way] - k)

    def relays_b(u, k, s):
        for way in range(2):
            when(place[way] >= k, relay_b, u, way, place[way] - k, s)

    def sent(like, sem):
        pltpu.make_async_remote_copy(like, like, sem, sem, device_id=other, device_id_type=MESH).wait_send()

    def free_x(u):
        sent(xa.at[0, 0], xa_send.at[u])
        sent(xb.at[0, 0], xb_send.at[u])

    def free_y(u):
        sent(out_y.at[0], y_send.at[u])

    early = [(LAG + f, hops_a, f) for f in range(3)] + [(f, hops_b, f) for f in range(3)]
    early = early[::-1] if B_FIRST else early
    early += [(LAG + 3 + k, relays_a, k) for k in range(1, 4)]
    early += [(LAG + 3, step_a), (3, line_b)]
    middle = [(LAG - 8 + b, sum_t, b) for b in range(4)]
    middle += [(-4, sum_b, 0, 2), (-3, sum_b, 2, 2), (LAG - 1, sum_a, 0, 4)]
    middle += [(-16, to_partner), (LAG - 9, load_t), (-7, load_b), (LAG - 2, load_a), (1, load_state), (8, free_x), (3, free_y)]
    late = [(B_OWN + k, relays_b, k, 0) for k in range(1, 4)] + [(B_OTHER + k, relays_b, k, 1) for k in range(1, 4)]
    late += [(B_STEP, step_b)] + ([(B_OWN, own_b_out)] if B_OWN != B_STEP else []) + [(B_OTHER, from_across_b), (HAND, hand_over)]

    to_partner(0)

    def period(r, _):
        for f in range(4):
            for offset, body, *rest in early + middle + late:
                if offset % 4 == f:
                    u = r - offset // 4
                    when(jnp.logical_and(u >= 0, u < UNITS), body, u, *rest)
        return 0

    lax.fori_loop(0, UNITS + 3 + HAND // 4, lambda n, _: period(n - 3, _), 0)

    inner = lax.div(z + 1, 2) == 1

    def drain(u, _):
        sent(partner.at[u], pair_send.at[u])
        sent(out_z.at[u], z_send.at[u])
        sent(w_own.at[pl.ds(0, 4), pl.ds(0, GA)], ya_send.at[u])
        sent(w_own.at[u, pl.ds(GA, GB)], yb_send.at[u])
        sent(partner.at[u], hand_send.at[u])

        @pl.when(inner)
        def _():
            sent(w_own.at[pl.ds(0, 5), pl.ds(0, GA)], ga_send.at[u])
            sent(w_own.at[pl.ds(0, 10), pl.ds(GA, GB)], gb_send.at[u])

        @pl.when(jnp.logical_not(inner))
        def _():
            sent(w_own.at[0, pl.ds(0, GA)], ga_send.at[u])
            sent(w_own.at[pl.ds(0, 2), pl.ds(GA, GB)], gb_send.at[u])

        arrived(partner.at[u], hand_recv.at[u])
        return 0

    lax.fori_loop(0, UNITS, drain, 0)


def unload(gate, up, down, mv, *refs):
    new_w, new_m, new_v = refs[:3], refs[3:6], refs[6:9]
    slots, in_sem, out_sem, down_sem, mv_sem = refs[9:]
    chunks = [(which, layer, row, half) for which in range(2) for layer in range(2) for row in range(2) for half in range(2)]
    sources = (gate, up, down)

    def read(n):
        which, layer, row, half = chunks[n]
        return pltpu.make_async_copy(sources[which].at[layer, row, pl.ds(2 * half, 2)], slots.at[n % SLOTS], in_sem.at[n % SLOTS])

    def write(n):
        which, layer, row, half = chunks[n]
        return pltpu.make_async_copy(slots.at[n % SLOTS], new_w[which].at[layer, row, pl.ds(2 * half, 2)], out_sem.at[n % SLOTS])

    for n in range(SLOTS):
        read(n).start()
    pltpu.make_async_copy(down, new_w[2], down_sem).start()
    for u in range(UNITS):
        which, layer, q = u // 8, u // 4 % 2, u % 4
        for i, to in enumerate((new_m, new_v)):
            target = to[which].at[layer, q] if which == 2 else to[which].at[layer, :, pl.ds(q * LANES, LANES)]
            pltpu.make_async_copy(mv.at[u, i], target, mv_sem).start()
    for n in range(len(chunks)):
        read(n).wait()
        write(n).start()
        ahead = n + SLOTS - 2
        if n >= 2 and ahead < len(chunks):
            write(ahead - SLOTS).wait()
            read(ahead).start()
    for n in range(len(chunks) - SLOTS, len(chunks)):
        write(n).wait()
    pltpu.make_async_copy(down, down, down_sem).wait()
    pltpu.make_async_copy(mv, mv, mv_sem).wait()


def solution(mesh):
    def step(*arrays):
        def split(i, a):
            if i % 3 == 2:
                return a.reshape(2, 2, 4, 2, 4, ROWS, LANES)
            return a.reshape(2, 2, 4, 2, ROWS, 4 * LANES)

        whole = [split(i, a) for i, a in enumerate(arrays[:6])]
        moments = [a if i % 3 < 2 else a.reshape(2, 4, ROWS, LANES) for i, a in enumerate(arrays[6:])]
        dma = pltpu.SemaphoreType.DMA
        by_unit = dma((UNITS,))
        hbm = [jax.ShapeDtypeStruct(a.shape, a.dtype) for a in whole[3:]]
        kept = [pltpu.VMEM(whole[5].shape, BF16), pltpu.VMEM((UNITS, 2, ROWS, LANES), F32)]
        out = pl.pallas_call(
            kernel,
            out_shape=(
                *hbm[:2],
                *kept,
                jax.ShapeDtypeStruct((UNITS, 2, 4, ROWS, LANES), BF16),
                jax.ShapeDtypeStruct((UNITS, 4, A, LANES), BF16),
            ),
            in_specs=[pl.BlockSpec(memory_space=pl.ANY)] * 12,
            out_specs=[pl.BlockSpec(memory_space=space) for space in (pl.ANY, pl.ANY, pltpu.VMEM, pltpu.VMEM, pl.ANY, pl.ANY)],
            scratch_shapes=[
                pltpu.VMEM((RING, 2, 3, A, LANES), BF16),
                pltpu.VMEM((RING, 2, 3, 2, B, LANES), BF16),
                pltpu.VMEM((RING, 4, A, LANES), BF16),
                pltpu.VMEM((UNITS, B, LANES), BF16),
                pltpu.VMEM((UNITS, B, LANES), BF16),
                pltpu.VMEM((3, 4, A, LANES), F32),
                pltpu.VMEM((3, 4, 2, B, LANES), F32),
                pltpu.VMEM((2, 4, A, LANES), BF16),
                pltpu.VMEM((3, 4, A, LANES), BF16),
                pltpu.VMEM((2, 2, 4, B, LANES), BF16),
                pltpu.VMEM((UNITS, ROWS, LANES), BF16),
                *(by_unit, by_unit),
                *(dma((2,)), dma((3,)), dma((2,)), *(dma((3,)),) * 2, by_unit, by_unit),
                *(by_unit,) * 4,
                *(by_unit, dma((UNITS, 2, 3)), by_unit, dma((UNITS, 2, 3))),
                *(by_unit, dma((UNITS, 2, 3)), by_unit, dma((UNITS, 2, 3, 2))),
                *(by_unit,) * 6,
            ],
            compiler_params=pltpu.CompilerParams(collective_id=0, has_side_effects=True, vmem_limit_bytes=24 * 1024 * 1024),
        )(*whole, *moments)
        final = pl.pallas_call(
            unload,
            out_shape=(*hbm, *(jax.ShapeDtypeStruct(a.shape, a.dtype) for a in moments)),
            in_specs=[pl.BlockSpec(memory_space=space) for space in (pltpu.HBM, pltpu.HBM, pltpu.VMEM, pltpu.VMEM)],
            out_specs=[pl.BlockSpec(memory_space=pl.ANY)] * 9,
            scratch_shapes=[pltpu.VMEM((SLOTS, 2, 2, ROWS, 4 * LANES), BF16), dma((SLOTS,)), dma((SLOTS,)), dma, dma],
            compiler_params=pltpu.CompilerParams(vmem_limit_bytes=24 * 1024 * 1024),
        )(*(pltpu.with_memory_space_constraint(a, space) for a, space in zip(out[:4], (pltpu.HBM, pltpu.HBM, pltpu.VMEM, pltpu.VMEM), strict=True)))
        return tuple(a.reshape(like.shape) for a, like in zip(final, arrays[3:], strict=True))

    all_of, cut = P(None, None, None), P(None, "dp", None)
    return jax.shard_map(
        step,
        mesh=mesh,
        in_specs=(P(("rep", "dp"), None, None, None),) * 3 + (all_of,) * 3 + (cut,) * 6,
        out_specs=(P("rep", None, None),) * 3 + (P("rep", "dp", None),) * 6,
        check_vma=False,
    )
```

```python
import jax
import jax.numpy as jnp
from jax import lax
from jax.experimental import pallas as pl
from jax.experimental.pallas import tpu as pltpu
from jax.sharding import PartitionSpec as P

F32, BF16 = jnp.float32, jnp.bfloat16
MESH = pl.DeviceIdType.MESH
UNITS = 24
RING, SLOTS = 4, 8
ROWS, A, B, LANES = 72, 40, 32, 1152
GA, GB = 48, 24
LAG, B_STEP, B_OWN, B_OTHER, HAND, B_FIRST = 2, 4, 4, 5, 10, False


def lanes(body):
    def at(j, _):
        body(pl.ds(pl.multiple_of(j * 384, 384), 384))
        return 0

    lax.fori_loop(0, 3, at, 0)


def kernel(*refs):
    terms, weights, ms, vs = (refs[i : i + 3] for i in (0, 3, 6, 9))
    new_w = refs[12:15]
    mv, partner, over_y = refs[15:18]
    xa, xb, out_y, out_z, in_z, la, lb, t_in, a_in, b_in, w_own = refs[18:29]
    (
        pair_send, pair_recv, t_load, a_load, b_load, mv_load, w_load, own_a, own_b,
        y_send, y_recv, z_send, z_recv, xa_send, xa_recv, xb_send, xb_recv,
        ga_send, ga_recv, gb_send, gb_recv, ya_send, ya_recv, yb_send, yb_recv, hand_send, hand_recv,
    ) = refs[29:]

    me = lax.axis_index("dp")
    core = lax.rem(me, 2)
    z = lax.rem(lax.div(me, 2), 4)
    y = lax.div(me, 8)
    other = {"dp": me + 1 - 2 * core}
    across = {"dp": me + 8 - 16 * y}
    ahead = ({"dp": me + 2}, {"dp": me - 2})
    place = (z, 3 - z)

    barrier = pltpu.get_barrier_semaphore()
    for device in (other, across):
        pl.semaphore_signal(barrier, inc=1, device_id=device, device_id_type=MESH)
    for way in range(2):

        @pl.when(place[way] < 3)
        def _(way=way):
            pl.semaphore_signal(barrier, inc=1, device_id=ahead[way], device_id_type=MESH)

    pl.semaphore_wait(barrier, 2 + lax.div(z + 2, 3) + lax.div(5 - z, 3))

    def z_of(way, b):
        return b if way == 0 else 3 - b

    def each(u, body):
        for which in range(3):

            @pl.when(lax.div(u, 8) == which)
            def _(which=which):
                body(which, lax.rem(lax.div(u, 4), 2), lax.rem(u, 4))

    def cut(ref, which, lead, q, first, count):
        if which == 2:
            return ref.at[(*lead, q, pl.ds(first, count))]
        return ref.at[(*lead, pl.ds(first, count), pl.ds(pl.multiple_of(q * LANES, 128), LANES))]

    def send(source, target, sent, received, device):
        pltpu.make_async_remote_copy(source, target, sent, received, device_id=device, device_id_type=MESH).start()

    def arrived(like, sem, device=other):
        pltpu.make_async_remote_copy(like, like, sem, sem, device_id=device, device_id_type=MESH).wait_recv()

    def copied(like, sem):
        pltpu.make_async_copy(like, like, sem).wait()

    def to_partner(u):
        def go(which, layer, q):
            source = cut(terms[which], which, (layer, slice(None), slice(None), 1 - core), q, 0, ROWS)
            send(source, partner.at[u], pair_send.at[u], pair_recv.at[u], other)

        each(u, go)

    def load_t(u):
        arrived(partner.at[u], pair_recv.at[u])

        def go(which, layer, q):
            source = cut(terms[which], which, (layer, 1 - y, slice(None), core), q, 0, A)
            pltpu.make_async_copy(source, t_in.at[0], t_load.at[0]).start()

        each(u, go)
        pltpu.make_async_copy(partner.at[u, 1 - y, :, pl.ds(0, A)], t_in.at[1], t_load.at[1]).start()

    def sum_t(u, b):
        if b == 0:
            for i in range(2):
                copied(t_in.at[i], t_load.at[i])

        def body(c):
            out_y[lax.rem(u, RING), b, :, c] = (t_in[0, b, :, c].astype(F32) + t_in[1, b, :, c].astype(F32)).astype(BF16)

        lanes(body)
        send(out_y.at[lax.rem(u, RING), b], over_y.at[u, b], y_send.at[u], y_recv.at[u], across)

    def load_a(u):
        arrived(over_y.at[u], y_recv.at[u], across)

        def go(which, layer, q):
            source = cut(terms[which], which, (layer, y, slice(None), core), q, 0, A)
            pltpu.make_async_copy(source, a_in.at[0], a_load.at[0]).start()

        each(u, go)
        pltpu.make_async_copy(partner.at[u, y, :, pl.ds(0, A)], a_in.at[1], a_load.at[1]).start()
        pltpu.make_async_copy(over_y.at[u], a_in.at[2], a_load.at[2]).start()

    def sum_a(u, first, count):
        if first == 0:
            for i in range(3):
                copied(a_in.at[i], a_load.at[i])

        def one(b, _):
            def body(c):
                la[lax.rem(u, 3), b, :, c] = (
                    a_in[0, b, :, c].astype(F32) + a_in[1, b, :, c].astype(F32) + a_in[2, b, :, c].astype(F32)
                )

            lanes(body)
            return 0

        lax.fori_loop(first, first + count, one, 0)

    def load_b(u):
        def go(which, layer, q):
            source = cut(terms[which], which, (layer, slice(None), slice(None), core), q, A, B)
            pltpu.make_async_copy(source, b_in.at[0], b_load.at[0]).start()

        each(u, go)
        pltpu.make_async_copy(partner.at[u, :, :, pl.ds(A, B)], b_in.at[1], b_load.at[1]).start()

    def sum_b(u, first, count):
        if first == 0:
            for i in range(2):
                copied(b_in.at[i], b_load.at[i])

        def one(n, _):
            b, s = lax.div(n, 2), lax.rem(n, 2)

            def body(c):
                lb[lax.rem(u, 3), b, s, :, c] = b_in[0, s, b, :, c].astype(F32) + b_in[1, s, b, :, c].astype(F32)

            lanes(body)
            return 0

        lax.fori_loop(2 * first, 2 * (first + count), one, 0)

    def hop_a(u, way, b):
        i = place[way]
        x = xa.at[lax.rem(u, RING), way, b - 1]
        mine = la.at[lax.rem(u, 3), z_of(way, b)]

        @pl.when(i == 0)
        def _():
            def body(c):
                x[:, c] = mine[:, c].astype(BF16)

            lanes(body)

        @pl.when(i > 0)
        def _():
            arrived(x, xa_recv.at[u, way, b - 1])

            def body(c):
                x[:, c] = (mine[:, c] + x[:, c].astype(F32)).astype(BF16)

            lanes(body)

        send(x, x, xa_send.at[u], xa_recv.at[u, way, b - 1], ahead[way])

    def hop_b(u, way, b):
        i = place[way]
        x = xb.at[lax.rem(u, RING), way, b - 1]
        mine = lb.at[lax.rem(u, 3), z_of(way, b)]

        @pl.when(i == 0)
        def _():
            def body(c):
                for s in range(2):
                    x[s, :, c] = mine[s, :, c].astype(BF16)

            lanes(body)

        @pl.when(i > 0)
        def _():
            arrived(x, xb_recv.at[u, way, b - 1])

            def body(c):
                for s in range(2):
                    x[s, :, c] = (mine[s, :, c] + x[s, :, c].astype(F32)).astype(BF16)

            lanes(body)

        send(x, x, xb_send.at[u], xb_recv.at[u, way, b - 1], ahead[way])

    def load_state(u):
        def go(which, layer, q):
            for i, from_ in enumerate((ms, vs)):
                source = cut(from_[which], which, (layer,), q, 0, ROWS)
                pltpu.make_async_copy(source, mv.at[u, i], mv_load.at[lax.rem(u, 3)]).start()
            source = cut(weights[which], which, (layer, y, z, core), q, 0, ROWS)
            pltpu.make_async_copy(source, w_own.at[u], w_load.at[lax.rem(u, 3)]).start()

        each(u, go)

    def adamw(g, u, first, count, c):
        rows = pl.ds(first, count)
        w_ref, m_ref, v_ref = w_own.at[u], mv.at[u, 0], mv.at[u, 1]
        g = g.astype(BF16).astype(F32)
        w = w_ref[rows, c].astype(F32)
        m = 0.9 * m_ref[rows, c] + 0.1 * g
        v = 0.95 * v_ref[rows, c] + 0.05 * g * g
        step = m * lax.rsqrt(v + 1e-8) + 0.1 * w
        w_ref[rows, c] = (w - 0.02 * step).astype(BF16)
        m_ref[rows, c] = m
        v_ref[rows, c] = v

    def spread(which, layer, q, u, first, count, own_sem, across_sent, across_received, line_sent, line_received):
        where = cut(new_w[which], which, (layer, y, z, core), q, first, count)
        source = w_own.at[u, pl.ds(first, count)]
        if line_sent is not None:
            for way in range(2):

                @pl.when(place[way] < 3)
                def _(way=way):
                    send(source, where, line_sent.at[u], line_received(way), ahead[way])

        send(source, where, across_sent.at[u], across_received.at[u], across)
        pltpu.make_async_copy(source, where, own_sem.at[u]).start()

    def step_a(u):
        mine = la.at[lax.rem(u, 3), z]
        for way in range(2):

            @pl.when(place[way] > 0)
            def _(way=way):
                x = xa.at[lax.rem(u, RING), way, place[way] - 1]
                arrived(x, xa_recv.at[u, way, place[way] - 1])

                def body(c):
                    mine[:, c] = mine[:, c] + x[:, c].astype(F32)

                lanes(body)

        lanes(lambda c: adamw(mine[:, c], u, 0, A, c))

        def go(which, layer, q):
            spread(which, layer, q, u, 0, GA, own_a, ya_send, ya_recv, ga_send, lambda way: ga_recv.at[u, way, place[way]])

        each(u, go)

    def line_b(u):
        copied(mv.at[u], mv_load.at[lax.rem(u, 3)])
        copied(w_own.at[u], w_load.at[lax.rem(u, 3)])
        mine = lb.at[lax.rem(u, 3), z]
        for way in range(2):

            @pl.when(place[way] > 0)
            def _(way=way):
                x = xb.at[lax.rem(u, RING), way, place[way] - 1]
                arrived(x, xb_recv.at[u, way, place[way] - 1])

                def body(c):
                    for s in range(2):
                        mine[s, :, c] = mine[s, :, c] + x[s, :, c].astype(F32)

                lanes(body)

        def body(c):
            out_z[u, :, c] = mine[1 - y, :, c].astype(BF16)

        lanes(body)
        send(out_z.at[u], in_z.at[u], z_send.at[u], z_recv.at[u], across)

    def step_b(u):
        arrived(in_z.at[u], z_recv.at[u], across)
        mine = lb.at[lax.rem(u, 3), z]
        lanes(lambda c: adamw(mine[y, :, c] + in_z[u, :, c].astype(F32), u, A, B, c))

        def go(which, layer, q):
            spread(which, layer, q, u, GA, GB, own_b, yb_send, yb_recv, gb_send if B_OWN == B_STEP else None, lambda way: gb_recv.at[u, way, place[way], 0])

        each(u, go)

    def relay_a(u, way, b):
        arrived(w_own.at[u, pl.ds(0, GA)], ga_recv.at[u, way, b])

        def go(which, layer, q):
            where = cut(new_w[which], which, (layer, y, z_of(way, b), core), q, 0, GA)

            @pl.when(place[way] < 3)
            def _():
                send(where, where, ga_send.at[u], ga_recv.at[u, way, b], ahead[way])

            send(where, where, ya_send.at[u], ya_recv.at[u], across)

        each(u, go)

    def relay_b(u, way, b, s):
        arrived(w_own.at[u, pl.ds(GA, GB)], gb_recv.at[u, way, b, s])

        @pl.when(place[way] < 3)
        def _():
            def go(which, layer, q):
                row = y if s == 0 else 1 - y
                where = cut(new_w[which], which, (layer, row, z_of(way, b), core), q, GA, GB)
                send(where, where, gb_send.at[u], gb_recv.at[u, way, b, s], ahead[way])

            each(u, go)

    def own_b_out(u):
        def go(which, layer, q):
            where = cut(new_w[which], which, (layer, y, z, core), q, GA, GB)
            for way in range(2):

                @pl.when(place[way] < 3)
                def _(way=way):
                    send(w_own.at[u, pl.ds(GA, GB)], where, gb_send.at[u], gb_recv.at[u, way, place[way], 0], ahead[way])

        each(u, go)

    def from_across_b(u):
        arrived(w_own.at[u, pl.ds(GA, GB)], yb_recv.at[u], across)

        def go(which, layer, q):
            where = cut(new_w[which], which, (layer, 1 - y, z, core), q, GA, GB)
            for way in range(2):

                @pl.when(place[way] < 3)
                def _(way=way):
                    send(where, where, gb_send.at[u], gb_recv.at[u, way, place[way], 1], ahead[way])

        each(u, go)

    def hand_over(u):
        arrived(w_own.at[pl.ds(0, 4), pl.ds(0, GA)], ya_recv.at[u], across)
        copied(w_own.at[u, pl.ds(0, GA)], own_a.at[u])
        copied(w_own.at[u, pl.ds(GA, GB)], own_b.at[u])

        def go(which, layer, q):
            where = cut(new_w[which], which, (layer, slice(None), slice(None), core), q, 0, ROWS)
            send(where, where, hand_send.at[u], hand_recv.at[u], other)

        each(u, go)

    def when(condition, body, *args):
        @pl.when(condition)
        def _():
            body(*args)

    def hops_a(u, f):
        for way in range(2):
            when(place[way] <= f, hop_a, u, way, 3 - f + place[way])

    def hops_b(u, f):
        for way in range(2):
            when(place[way] <= f, hop_b, u, way, 3 - f + place[way])

    def relays_a(u, k):
        for way in range(2):
            when(place[way] >= k, relay_a, u, way, place[way] - k)

    def relays_b(u, k, s):
        for way in range(2):
            when(place[way] >= k, relay_b, u, way, place[way] - k, s)

    def sent(like, sem):
        pltpu.make_async_remote_copy(like, like, sem, sem, device_id=other, device_id_type=MESH).wait_send()

    def free_x(u):
        sent(xa.at[0, 0], xa_send.at[u])
        sent(xb.at[0, 0], xb_send.at[u])

    def free_y(u):
        sent(out_y.at[0], y_send.at[u])

    early = [(LAG + f, hops_a, f) for f in range(3)] + [(f, hops_b, f) for f in range(3)]
    early = early[::-1] if B_FIRST else early
    early += [(LAG + 3, step_a), (3, line_b)]
    middle = [(LAG - 8 + b, sum_t, b) for b in range(4)]
    middle += [(-4, sum_b, 0, 2), (-3, sum_b, 2, 2), (LAG - 1, sum_a, 0, 4)]
    middle += [(-16, to_partner), (LAG - 9, load_t), (-7, load_b), (LAG - 2, load_a), (1, load_state), (8, free_x), (3, free_y)]
    late = [(B_OWN + k, relays_b, k, 0) for k in range(1, 4)] + [(B_OTHER + k, relays_b, k, 1) for k in range(1, 4)]
    late = [(LAG + 3 + k, relays_a, k) for k in range(1, 4)] + late
    late += [(B_STEP, step_b)] + ([(B_OWN, own_b_out)] if B_OWN != B_STEP else []) + [(B_OTHER, from_across_b), (HAND, hand_over)]

    to_partner(0)

    def period(r, _):
        for f in range(4):
            for offset, body, *rest in early + middle + late:
                if offset % 4 == f:
                    u = r - offset // 4
                    when(jnp.logical_and(u >= 0, u < UNITS), body, u, *rest)
        return 0

    lax.fori_loop(0, UNITS + 3 + HAND // 4, lambda n, _: period(n - 3, _), 0)

    inner = lax.div(z + 1, 2) == 1

    def drain(u, _):
        sent(partner.at[u], pair_send.at[u])
        sent(out_z.at[u], z_send.at[u])
        sent(w_own.at[pl.ds(0, 4), pl.ds(0, GA)], ya_send.at[u])
        sent(w_own.at[u, pl.ds(GA, GB)], yb_send.at[u])
        sent(partner.at[u], hand_send.at[u])

        @pl.when(inner)
        def _():
            sent(w_own.at[pl.ds(0, 5), pl.ds(0, GA)], ga_send.at[u])
            sent(w_own.at[pl.ds(0, 10), pl.ds(GA, GB)], gb_send.at[u])

        @pl.when(jnp.logical_not(inner))
        def _():
            sent(w_own.at[0, pl.ds(0, GA)], ga_send.at[u])
            sent(w_own.at[pl.ds(0, 2), pl.ds(GA, GB)], gb_send.at[u])

        arrived(partner.at[u], hand_recv.at[u])
        return 0

    lax.fori_loop(0, UNITS, drain, 0)


def unload(gate, up, down, mv, *refs):
    new_w, new_m, new_v = refs[:3], refs[3:6], refs[6:9]
    slots, in_sem, out_sem, down_sem, mv_sem = refs[9:]
    chunks = [(which, layer, row, half) for which in range(2) for layer in range(2) for row in range(2) for half in range(2)]
    sources = (gate, up, down)

    def read(n):
        which, layer, row, half = chunks[n]
        return pltpu.make_async_copy(sources[which].at[layer, row, pl.ds(2 * half, 2)], slots.at[n % SLOTS], in_sem.at[n % SLOTS])

    def write(n):
        which, layer, row, half = chunks[n]
        return pltpu.make_async_copy(slots.at[n % SLOTS], new_w[which].at[layer, row, pl.ds(2 * half, 2)], out_sem.at[n % SLOTS])

    for n in range(SLOTS):
        read(n).start()
    for n in range(len(chunks)):
        read(n).wait()
        write(n).start()
        if n == 5:
            pltpu.make_async_copy(down, new_w[2], down_sem).start()
            for u in range(UNITS):
                which, layer, q = u // 8, u // 4 % 2, u % 4
                for i, to in enumerate((new_m, new_v)):
                    target = to[which].at[layer, q] if which == 2 else to[which].at[layer, :, pl.ds(q * LANES, LANES)]
                    pltpu.make_async_copy(mv.at[u, i], target, mv_sem).start()
        ahead = n + SLOTS - 2
        if n >= 2 and ahead < len(chunks):
            write(ahead - SLOTS).wait()
            read(ahead).start()
    for n in range(len(chunks) - SLOTS, len(chunks)):
        write(n).wait()
    pltpu.make_async_copy(down, down, down_sem).wait()
    pltpu.make_async_copy(mv, mv, mv_sem).wait()


def solution(mesh):
    def step(*arrays):
        def split(i, a):
            if i % 3 == 2:
                return a.reshape(2, 2, 4, 2, 4, ROWS, LANES)
            return a.reshape(2, 2, 4, 2, ROWS, 4 * LANES)

        whole = [split(i, a) for i, a in enumerate(arrays[:6])]
        moments = [a if i % 3 < 2 else a.reshape(2, 4, ROWS, LANES) for i, a in enumerate(arrays[6:])]
        dma = pltpu.SemaphoreType.DMA
        by_unit = dma((UNITS,))
        hbm = [jax.ShapeDtypeStruct(a.shape, a.dtype) for a in whole[3:]]
        kept = [pltpu.VMEM(whole[5].shape, BF16), pltpu.VMEM((UNITS, 2, ROWS, LANES), F32)]
        out = pl.pallas_call(
            kernel,
            out_shape=(
                *hbm[:2],
                *kept,
                jax.ShapeDtypeStruct((UNITS, 2, 4, ROWS, LANES), BF16),
                jax.ShapeDtypeStruct((UNITS, 4, A, LANES), BF16),
            ),
            in_specs=[pl.BlockSpec(memory_space=pl.ANY)] * 12,
            out_specs=[pl.BlockSpec(memory_space=space) for space in (pl.ANY, pl.ANY, pltpu.VMEM, pltpu.VMEM, pl.ANY, pl.ANY)],
            scratch_shapes=[
                pltpu.VMEM((RING, 2, 3, A, LANES), BF16),
                pltpu.VMEM((RING, 2, 3, 2, B, LANES), BF16),
                pltpu.VMEM((RING, 4, A, LANES), BF16),
                pltpu.VMEM((UNITS, B, LANES), BF16),
                pltpu.VMEM((UNITS, B, LANES), BF16),
                pltpu.VMEM((3, 4, A, LANES), F32),
                pltpu.VMEM((3, 4, 2, B, LANES), F32),
                pltpu.VMEM((2, 4, A, LANES), BF16),
                pltpu.VMEM((3, 4, A, LANES), BF16),
                pltpu.VMEM((2, 2, 4, B, LANES), BF16),
                pltpu.VMEM((UNITS, ROWS, LANES), BF16),
                *(by_unit, by_unit),
                *(dma((2,)), dma((3,)), dma((2,)), *(dma((3,)),) * 2, by_unit, by_unit),
                *(by_unit,) * 4,
                *(by_unit, dma((UNITS, 2, 3)), by_unit, dma((UNITS, 2, 3))),
                *(by_unit, dma((UNITS, 2, 3)), by_unit, dma((UNITS, 2, 3, 2))),
                *(by_unit,) * 6,
            ],
            compiler_params=pltpu.CompilerParams(collective_id=0, has_side_effects=True, vmem_limit_bytes=24 * 1024 * 1024),
        )(*whole, *moments)
        final = pl.pallas_call(
            unload,
            out_shape=(*hbm, *(jax.ShapeDtypeStruct(a.shape, a.dtype) for a in moments)),
            in_specs=[pl.BlockSpec(memory_space=space) for space in (pltpu.HBM, pltpu.HBM, pltpu.VMEM, pltpu.VMEM)],
            out_specs=[pl.BlockSpec(memory_space=pl.ANY)] * 9,
            scratch_shapes=[pltpu.VMEM((SLOTS, 2, 2, ROWS, 4 * LANES), BF16), dma((SLOTS,)), dma((SLOTS,)), dma, dma],
            compiler_params=pltpu.CompilerParams(vmem_limit_bytes=24 * 1024 * 1024),
        )(*(pltpu.with_memory_space_constraint(a, space) for a, space in zip(out[:4], (pltpu.HBM, pltpu.HBM, pltpu.VMEM, pltpu.VMEM), strict=True)))
        return tuple(a.reshape(like.shape) for a, like in zip(final, arrays[3:], strict=True))

    all_of, cut = P(None, None, None), P(None, "dp", None)
    return jax.shard_map(
        step,
        mesh=mesh,
        in_specs=(P(("rep", "dp"), None, None, None),) * 3 + (all_of,) * 3 + (cut,) * 6,
        out_specs=(P("rep", None, None),) * 3 + (P("rep", "dp", None),) * 6,
        check_vma=False,
    )
```
